32 devices in a mesh: tm: 8 (over z, y), space: 4 (over x, core).
Axes of the slice: x: 2, y: 2, z: 4, core: 2. Of those that a mesh axis runs over, the one named last changes fastest.
Arguments:
- density: bfloat16 [2048, 128, 128], P('tm', 'space'), may hold values from -6 to 6
- active: int32 [2048], P('tm'), may hold values from 1 to 128
- neighbours: int32 [128, 8], P('space'), may hold values from 0 to 127, as said below
- near_blocks: bfloat16 [2, 128, 8, 128, 128], P(None, 'space'), may hold values from -0.125 to 0.125
- to_moments: bfloat16 [64, 128, 128], P(None, 'space'), may hold values from -0.046875 to 0.046875
- from_moments: bfloat16 [64, 128, 128], P(None, 'space'), may hold values from -0.75 to 0.75
- decay_rates: float32 [64], replicated, may hold values from 9.765625e-05 to 0.05, as said below
- lengths: float32 [2048], P('tm'), may hold values from 0.5 to 1024, as said below
Outputs:
- potential: bfloat16 [2048, 128, 128], P('tm', 'space')
The draws below stay inside these ranges and needn't reach their ends.
Inputs may be any that keep to these rules, and one draw needn't show every extreme that they name: `neighbours`: every entry of row c lies within 8 of c; each row names c - 8 and c + 8, clipped to the clusters that exist. `decay_rates`: positive rates. Positive lengths.
All inputs are finite; a program needn't handle non-finite values.
Results may differ from the reference program's by a relative error of at most 0.0085.
Values may be sent and summed in bfloat16 or wider, within the bound.
A program may use at most 128 MiB of HBM per device.

```python
import jax
import jax.numpy as jnp
from jax import lax

ELEM = 128
TERMS = 64
NB = 8
REACH = 8
NT = 2048
NC = 128


def draw_neighbours(key, part):
    offsets = jax.random.randint(key, (NC, NB), -REACH, REACH + 1)
    scores = jax.random.randint(jax.random.fold_in(key, 3), (NC, NB), 0, 1 << 20) * NB + jnp.arange(NB, dtype=jnp.int32)[None, :]
    order = jnp.argsort(scores, axis=1)
    ranks = jnp.argsort(order, axis=1)
    offsets = jnp.where(ranks == 0, REACH, jnp.where(ranks == 1, -REACH, offsets))
    result = jnp.clip(jnp.arange(NC, dtype=jnp.int32)[:, None] + offsets, 0, NC - 1)
    return result.astype(jnp.int32)


def draw_decay_rates(key, part):
    pick = jax.random.uniform(jax.random.fold_in(key, 11), (TERMS,))
    share = 0.5
    slow_log = jax.random.uniform(jax.random.fold_in(key, 12), (TERMS,), minval=jnp.log(0.2 / NT), maxval=jnp.log(0.8 / NT))
    fast_log = jax.random.uniform(jax.random.fold_in(key, 13), (TERMS,), minval=jnp.log(0.02), maxval=jnp.log(0.05))
    return jnp.where(pick < share, jnp.exp(slow_log), jnp.exp(fast_log)).astype(jnp.float32)


def draw_lengths(key, part):
    base = jax.random.uniform(key, (NT,), minval=0.5, maxval=2.0)
    places = jax.random.randint(jax.random.fold_in(key, 5), (3,), 0, NT)
    base = base.at[places].set(jnp.float32(NT // 2))
    return base.astype(jnp.float32)


def touch_ends(values, stream_key, low, high):
    spot = [jax.random.randint(jax.random.fold_in(stream_key, axis), (), 0, length) for axis, length in enumerate(values.shape)]
    longest = values.shape.index(max(values.shape))
    neighbour = spot[:longest] + [(spot[longest] + 1) % values.shape[longest]] + spot[longest + 1:]
    return values.at[tuple(spot)].set(low).at[tuple(neighbour)].set(high)


def levels(stream_key, dims, split, low, largest):
    loudness = 1.0
    for axis_at, parts in split:
        steps = jax.random.uniform(jax.random.fold_in(jax.random.fold_in(stream_key, 6), axis_at), (parts,), jnp.float32, low / len(split), largest / len(split))
        loudness = loudness * jnp.repeat(jnp.exp(steps), dims[axis_at] // parts).reshape((-1,) + (1,) * (len(dims) - 1 - axis_at))
    return loudness


def bell_draw(own_key, dims, deviation, bound, split=(), kind=jnp.bfloat16):
    factor_of = levels(own_key, dims, split, -0.22, 0.18) if split else 1.0
    values = jax.random.normal(own_key, dims, jnp.float32) * deviation * factor_of
    return jnp.minimum(jnp.maximum(values, -bound), bound).astype(kind)


def setup_inputs(seed: int = 0) -> dict:
    key_list = jax.random.split(jax.random.key(seed), 9)
    return {
        "density": bell_draw(key_list[0], (NT, NC, ELEM), 1.0, 6.0, ((0, 8), (1, 4))),
        "active": touch_ends(jax.random.randint(key_list[1], (NT,), 1, NC + 1), jax.random.fold_in(key_list[1], 1), 1, NC).astype(jnp.int32),
        "neighbours": draw_neighbours(jax.random.fold_in(key_list[8], 71), 0),
        "near_blocks": bell_draw(key_list[3], (2, NC, NB, ELEM, ELEM), (2 * NB * ELEM) ** -0.5, 0.125, ((1, 4),)),
        "to_moments": bell_draw(key_list[4], (TERMS, NC, ELEM), (NC * ELEM) ** -0.5, 0.046875, ((1, 4),)),
        "from_moments": bell_draw(key_list[5], (TERMS, NC, ELEM), TERMS ** -0.5, 0.75, ((1, 4),)),
        "decay_rates": draw_decay_rates(jax.random.fold_in(key_list[8], 71), 0),
        "lengths": draw_lengths(jax.random.fold_in(key_list[8], 71), 0),
    }


def reference(density, active, neighbours, near_blocks, to_moments, from_moments, decay_rates, lengths):
    live_mask = (jnp.arange(NC, dtype=jnp.int32)[None, :] < active[:, None]).astype(jnp.bfloat16)
    masked = density * live_mask[:, :, None]
    earlier = jnp.concatenate([jnp.zeros((1, NC, ELEM), jnp.bfloat16), masked[:-1]], 0)

    def one_cluster(cluster):
        chosen = neighbours[cluster]
        current = jnp.take(masked, chosen, axis=1).astype(jnp.float32)
        previous = jnp.take(earlier, chosen, axis=1).astype(jnp.float32)
        blocks = near_blocks[:, cluster].astype(jnp.float32)
        return jnp.einsum('tje,jef->tf', current, blocks[0]) + jnp.einsum('tje,jef->tf', previous, blocks[1])
    near_term = lax.map(one_cluster, jnp.arange(NC, dtype=jnp.int32))
    near_term = jnp.transpose(near_term, (1, 0, 2))
    flat = masked.reshape(NT, NC * ELEM)
    moments = jnp.dot(flat, to_moments.reshape(TERMS, NC * ELEM).T, preferred_element_type=jnp.float32)
    decays = jnp.exp(-decay_rates[None, :] * lengths[:, None])

    def advance(state, inputs):
        factor, moment = inputs
        return (factor * state + moment, state)
    _, far_coeff = lax.scan(advance, jnp.zeros((TERMS,), jnp.float32), (decays, moments))
    scaled = (far_coeff * jnp.sqrt(2.0 * decay_rates)[None, :]).astype(jnp.bfloat16)
    far_term = jnp.dot(scaled, from_moments.reshape(TERMS, NC * ELEM), preferred_element_type=jnp.float32)
    far_term = far_term.reshape(NT, NC, ELEM)
    return (live_mask.astype(jnp.float32)[:, :, None] * (near_term + far_term)).astype(jnp.bfloat16)
```

```python
import functools
import math

import jax
import jax.numpy as jnp
from jax import lax
from jax.experimental import pallas as pl
from jax.experimental.pallas import tpu as pltpu
from jax.sharding import PartitionSpec as P

REACH = 8
U = 8
DC = 4
PAD = 16
VMEM = 67043328
MESH = pl.DeviceIdType.MESH
F32, BF16 = jnp.float32, jnp.bfloat16


def spread(row):
    return jnp.broadcast_to(row, (128, row.shape[1])).T


def swap16():
    r = lax.broadcasted_iota(jnp.int32, (256, 256), 0)
    s = lax.broadcasted_iota(jnp.int32, (256, 256), 1)
    return jnp.where(s == (r % 16) * 16 + r // 16, 1.0, 0.0).astype(BF16)


def swap8():
    r = lax.broadcasted_iota(jnp.int32, (256, 256), 0)
    s = lax.broadcasted_iota(jnp.int32, (256, 256), 1)
    return jnp.where(s == (r % 32) * 8 + r // 32, 1.0, 0.0).astype(BF16)


def kernel(n_tm, n_space, dens, active_h, nbrs_h, blocks, to_m, from_m, rates_h, lengths_h,
           near, from_v, act, scaled_o, dens_v, work, active, nbrs, rates, lengths, perm, halo, halo_prev, row_out, row_in, wb, to_raw, from_raw, to_v,
           part_out, part_in, keep, tot_out, tot_in, state,
           in_sem, dens_sem, w_sem, halo_sem, row_sem, part_ssem, part_rsem, tot_ssem, tot_rsem):
    T, C, E = dens_v.shape
    M = to_raw.shape[0]
    J = wb.shape[2]
    H = T // 2
    tm, sp = lax.axis_index("tm"), lax.axis_index("space")
    first = sp * C

    TD = T // DC
    small = [pltpu.make_async_copy(a, b, in_sem.at[2 + i]) for i, (a, b) in enumerate(
        ((active_h, active), (nbrs_h, nbrs), (rates_h, rates), (lengths_h, lengths)))]
    c_to = pltpu.make_async_copy(to_m, to_raw, in_sem.at[0])
    c_from = pltpu.make_async_copy(from_m, from_raw, in_sem.at[1])

    def c_dens(k):
        return pltpu.make_async_copy(dens.at[pl.ds(k * TD, TD)], dens_v.at[pl.ds(k * TD, TD)], dens_sem.at[k])

    small[0].start()
    c_to.start()
    for k in range(DC):
        c_dens(k).start()
    for c in small[1:]:
        c.start()
    c_from.start()
    barrier = pltpu.get_barrier_semaphore()

    def greet(t, s):
        pl.semaphore_signal(barrier, inc=1, device_id={"tm": t, "space": s}, device_id_type=MESH)

    for d in range(1, n_space):
        greet(tm, lax.rem(sp + d, n_space))
    for d in range(1, n_tm):
        greet(lax.rem(tm + d, n_tm), sp)
    one, nil = jnp.int32(1), jnp.int32(0)
    has = {-1: (tm > 0, sp > 0), 1: (tm < n_tm - 1, sp < n_space - 1)}
    corners = nil
    for dt in (-1, 1):
        for ds in (-1, 1):
            there = jnp.logical_and(has[dt][0], has[ds][1])
            corners = corners + jnp.where(there, one, nil)

            @pl.when(there)
            def _(dt=dt, ds=ds):
                greet(tm + dt, sp + ds)

    def w_copy(c):
        return pltpu.make_async_copy(blocks.at[:, c], wb.at[:, c], w_sem.at[c])

    for lo, hi in ((REACH, C - REACH), (0, REACH), (C - REACH, C)):
        @pl.loop(lo, hi)
        def _(c):
            w_copy(c).start()

    perm[0] = swap16()
    perm[1] = swap8()
    small[0].wait()
    for h in range(2):
        act[h * H:(h + 1) * H, :] = spread(active[h:h + 1, :].astype(F32))

    def pair(raw, t, c0):
        x = [raw[pl.ds(t, 16), c0 + i * 16:c0 + i * 16 + 16, :].reshape(256, E) for i in range(2)]
        return jnp.dot(perm[0], jnp.concatenate(x, axis=1), preferred_element_type=F32)

    def expand(raw, dst):
        for b in range(M // 16):
            for c0 in range(0, C, 32):
                y = pair(raw, b * 16, c0).astype(BF16)
                for i in range(32):
                    x = y[i % 16 * 16:i % 16 * 16 + 16, i // 16 * E:(i // 16 + 1) * E]
                    dst[c0 + i, b * 16:b * 16 + 16, :] = x
                    dst[c0 + i, M + b * 16:M + b * 16 + 16, :] = x

    c_to.wait()
    expand(to_raw, to_v)
    for k in range(DC):
        c_dens(k).wait()

    gid = lax.broadcasted_iota(jnp.int32, (C, E), 0).astype(F32) + first.astype(F32)
    row_out[...] = jnp.where(gid < act[T - 1:T, :], dens_v[T - 1].astype(F32), 0.0)
    pl.semaphore_wait(barrier, n_space - 1 + n_tm - 1 + corners)

    def row_copy(ds):
        if ds == 0:
            src, dst = row_out, row_in.at[pl.ds(REACH, C)]
        elif ds == 1:
            src, dst = row_out.at[pl.ds(C - REACH, REACH)], row_in.at[pl.ds(0, REACH)]
        else:
            src, dst = row_out.at[pl.ds(0, REACH)], row_in.at[pl.ds(REACH + C, REACH)]
        return pltpu.make_async_remote_copy(
            src_ref=src, dst_ref=dst, send_sem=row_sem.at[0, ds + 1], recv_sem=row_sem.at[1, ds + 1],
            device_id={"tm": tm + 1, "space": sp + ds}, device_id_type=MESH)

    def halo_copy(ds, h):
        k = (1 - ds) // 2
        return pltpu.make_async_remote_copy(
            src_ref=dens_v.at[pl.ds(h * H, H), pl.ds(C - REACH if ds == 1 else 0, REACH), :],
            dst_ref=halo.at[k, pl.ds(h * H, H)],
            send_sem=halo_sem.at[0, k, h], recv_sem=halo_sem.at[1, k, h],
            device_id={"tm": tm, "space": sp + ds}, device_id_type=MESH)

    def halo_send(h):
        for ds in (1, -1):
            @pl.when(on_space(ds))
            def _(ds=ds):
                halo_copy(ds, h).start()

    def on_space(ds):
        return True if ds == 0 else has[ds][1]

    for ds in (0, 1, -1):
        @pl.when(jnp.logical_and(has[1][0], on_space(ds)))
        def _(ds=ds):
            row_copy(ds).start()
    halo_send(0)

    @pl.loop(0, T // 128)
    def _(b):
        for u in range(8):
            at = pl.multiple_of(b * 128 + u * 16, 16)
            live = act[pl.ds(at, 16), :]
            for c0 in range(0, C, 32):
                y = pair(dens_v, at, c0)
                for i in range(32):
                    x = y[i % 16 * 16:i % 16 * 16 + 16, i // 16 * E:(i // 16 + 1) * E]
                    x = jnp.where((first + (c0 + i)).astype(F32) < live, x, 0.0)
                    work[REACH + c0 + i, pl.ds(at, 16), :] = x.astype(BF16)

    lane = lax.broadcasted_iota(jnp.int32, (H, 2 * M), 1)
    low = lane < M
    total = jnp.zeros((T, 2 * M), F32)
    GB = 8
    for k in range(C // GB):
        a = jnp.concatenate([work[REACH + k * GB + i, 0:T, :] for i in range(GB)], axis=1)
        b = jnp.concatenate([to_v[k * GB + i] for i in range(GB)], axis=1)
        total = total + lax.dot_general(a, b, (((1,), (1,)), ((), ())), preferred_element_type=F32)
    part = jnp.where(low, total[0:H], total[H:T])
    keep[0] = part
    part_out[...] = part.astype(BF16)

    def part_copy(d):
        return pltpu.make_async_remote_copy(
            src_ref=part_out, dst_ref=part_in.at[sp], send_sem=part_ssem.at[d], recv_sem=part_rsem.at[sp],
            device_id={"tm": tm, "space": lax.rem(sp + d, n_space)}, device_id_type=MESH)

    for d in range(1, n_space):
        part_copy(d).start()
    halo_send(1)

    @pl.when(tm == 0)
    def _():
        row_in[...] = jnp.zeros_like(row_in)

    for ds in (0, 1, -1):
        there = has[-1][0] if ds == 0 else jnp.logical_and(has[-1][0], has[-ds][1])

        @pl.when(there)
        def _(ds=ds):
            row_copy(ds).wait_recv()
    top = lax.broadcasted_iota(jnp.int32, (PAD, E), 0) == 0

    @pl.loop(0, C + 2 * REACH)
    def _(g):
        r = jnp.broadcast_to(row_in[pl.ds(g, 1), :], (PAD, E))
        work[g, T:T + PAD, :] = jnp.where(top, r, 0.0).astype(BF16)

    first_row = lax.broadcasted_iota(jnp.int32, (T, E), 0) == 0

    small[1].wait()

    def near_field(c0):
        for u in range(U):
            w_copy(c0 + u).wait()
        for u in range(U):
            c = c0 + u
            rows = [jnp.clip(nbrs[j, c] - first + REACH, 0, C + 2 * REACH - 1) for j in range(J)]
            picked = jnp.concatenate([work[i] for i in rows], axis=1)
            w = jnp.concatenate([wb[0, c].reshape(J * E, E), wb[1, c].reshape(J * E, E)], axis=1)
            both = jnp.dot(picked, w, preferred_element_type=F32)
            late = both[:, E:]
            late = jnp.where(first_row, late[T:T + 1, :], pltpu.roll(late[0:T], 1, 0))
            near[c] = both[0:T, 0:E] + late

    @pl.loop(0, (C - 2 * REACH) // U)
    def _(i):
        near_field(REACH + i * U)

    moment = keep[0]
    for d in range(1, n_space):
        k = lax.rem(sp + n_space - d, n_space)
        pltpu.make_async_remote_copy(
            src_ref=part_out, dst_ref=part_in.at[k], send_sem=part_ssem.at[d], recv_sem=part_rsem.at[k],
            device_id={"tm": tm, "space": k}, device_id_type=MESH).wait_recv()
        moment = moment + part_in[k].astype(F32)
    small[2].wait()
    small[3].wait()
    r = rates[...]
    rr = jnp.concatenate([r, r], axis=1)
    span = jnp.where(low, spread(lengths[0:1, :]), spread(lengths[1:2, :]))
    fall = jnp.exp(-rr * span)
    pos = lax.broadcasted_iota(jnp.int32, (H, 2 * M), 0)
    d = 1
    while d < H:
        start = pos < d
        moment = fall * jnp.where(start, 0.0, pltpu.roll(moment, d, 0)) + moment
        fall = fall * jnp.where(start, 1.0, pltpu.roll(fall, d, 0))
        d *= 2
    keep[0] = jnp.where(pos < 1, 0.0, pltpu.roll(moment, 1, 0))
    keep[1] = jnp.where(pos < 1, 1.0, pltpu.roll(fall, 1, 0))
    end_b = jnp.broadcast_to(moment[H - 1:H, :], (8, 2 * M))
    end_a = jnp.broadcast_to(fall[H - 1:H, :], (8, 2 * M))
    low8 = low[0:8]
    roll_b, roll_a = pltpu.roll(end_b, M, 1), pltpu.roll(end_a, M, 1)
    tot_out[0:8] = end_a * roll_a
    tot_out[8:16] = jnp.where(low8, roll_a * end_b + roll_b, end_a * roll_b + end_b)

    def tot_copy(d):
        return pltpu.make_async_remote_copy(
            src_ref=tot_out, dst_ref=tot_in.at[tm], send_sem=tot_ssem.at[d], recv_sem=tot_rsem.at[tm],
            device_id={"tm": tm + d, "space": sp}, device_id_type=MESH)

    for d in range(1, n_tm):
        @pl.when(tm + d < n_tm)
        def _(d=d):
            tot_copy(d).start()

    c_from.wait()
    expand(from_raw, from_v)
    near_side = jnp.where(lax.rem(sp, 2) == 1, nil, one)
    for k in (near_side, one - near_side):
        other = sp + 2 * k - 1

        @pl.when(jnp.logical_and(other >= 0, other < n_space))
        def _(k=k, other=other):
            for h in range(2):
                pltpu.make_async_remote_copy(
                    src_ref=dens_v.at[pl.ds(h * H, H), pl.ds(0, REACH), :], dst_ref=halo.at[k, pl.ds(h * H, H)],
                    send_sem=halo_sem.at[0, k, h], recv_sem=halo_sem.at[1, k, h],
                    device_id={"tm": tm, "space": other}, device_id_type=MESH).wait_recv()

            begin = k * (REACH + C)

            for at in range(0, T, 64):
                x = [halo[k, pl.ds(at + i * 32, 32)].reshape(256, E) for i in range(2)]
                y = jnp.dot(perm[1], jnp.concatenate(x, axis=1), preferred_element_type=F32)
                for i in range(2):
                    live = act[pl.ds(at + i * 32, 32), :]
                    for g in range(REACH):
                        x = jnp.where((first - REACH + begin + g).astype(F32) < live,
                                      y[g * 32:g * 32 + 32, i * E:(i + 1) * E], 0.0)
                        work[begin + g, pl.ds(at + i * 32, 32), :] = x.astype(BF16)

        near_field(k * (C - REACH))

    state[...] = jnp.zeros_like(state)
    for k in range(n_tm - 1):
        @pl.when(k < tm)
        def _(k=k):
            pltpu.make_async_remote_copy(
                src_ref=tot_out, dst_ref=tot_in.at[k], send_sem=tot_ssem.at[0], recv_sem=tot_rsem.at[k],
                device_id={"tm": jnp.int32(k), "space": sp}, device_id_type=MESH).wait_recv()
            state[...] = tot_in[k, 0:8] * state[...] + tot_in[k, 8:16]
    s = state[...]
    arrive = jnp.where(low8, s, roll_a * s + roll_b)[0:1]
    scaled = (keep[1] * arrive + keep[0]) * jnp.sqrt(2.0 * rr)
    scaled_o[0:H] = jnp.where(low, scaled, 0.0).astype(BF16)
    scaled_o[H:T] = jnp.where(low, 0.0, scaled).astype(BF16)


    for d in range(1, n_space):
        part_copy(d).wait_send()
    for d in range(1, n_tm):
        @pl.when(tm + d < n_tm)
        def _(d=d):
            tot_copy(d).wait_send()
    for ds in (0, 1, -1):
        @pl.when(jnp.logical_and(has[1][0], on_space(ds)))
        def _(ds=ds):
            row_copy(ds).wait_send()
    for ds in (1, -1):
        @pl.when(on_space(ds))
        def _(ds=ds):
            for h in range(2):
                halo_copy(ds, h).wait_send()


def finish(near, from_v, act, scaled_o, out, stage, out_v, out_sem):
    C, T, E = near.shape
    GB = 8
    first = lax.axis_index("space") * C
    scaled = scaled_o[...]

    def out_copy(k):
        return pltpu.make_async_copy(out_v.at[k], out.at[:, pl.ds(k * GB, GB), :], out_sem.at[k])

    for k in range(C // GB):
        for i in range(0, GB, 2):
            g = k * GB + i
            far = jnp.dot(scaled, jnp.concatenate([from_v[g], from_v[g + 1]], axis=1), preferred_element_type=F32)
            for u in range(2):
                live = (first + g + u).astype(F32) < act[...]
                pot = jnp.where(live, near[g + u] + far[:, u * E:(u + 1) * E], 0.0)
                stage[pl.ds(i + u, T, stride=GB), :] = pot
        out_v[k] = stage[...].reshape(T, GB, E).astype(BF16)
        out_copy(k).start()
    for k in range(C // GB):
        out_copy(k).wait()


def solution(mesh):
    n_tm, n_space = mesh.shape["tm"], mesh.shape["space"]

    def local(density, active, neighbours, near_blocks, to_moments, from_moments, decay_rates, lengths):
        T, C, E = density.shape
        J = neighbours.shape[1]
        M = decay_rates.shape[0]
        H, W = T // 2, C + 2 * REACH
        vm = lambda shape, t: pltpu.VMEM(shape, t)
        dma = pltpu.SemaphoreType.DMA
        kept = [((C, T, E), F32), ((C, 2 * M, E), BF16), ((T, 128), F32), ((T, 2 * M), BF16)]
        room = sum(math.prod(s) * jnp.dtype(t).itemsize for s, t in kept) + 32 * 1024
        anyspec = pl.BlockSpec(memory_space=pl.ANY)
        vspec = pl.BlockSpec(memory_space=pltpu.VMEM)
        held = pl.pallas_call(
            functools.partial(kernel, n_tm, n_space),
            out_shape=[pltpu.VMEM(s, t) for s, t in kept],
            in_specs=[anyspec] * 8,
            out_specs=[vspec] * 4,
            scratch_shapes=[
                vm((T, C, E), BF16), vm((W, T + PAD, E), BF16),
                vm((2, H), jnp.int32), pltpu.SMEM((J, C), jnp.int32), vm((1, M), F32), vm((2, H), F32),
                vm((2, 256, 256), BF16),
                vm((2, T, REACH, E), BF16), vm((8, 128), F32), vm((C, E), F32), vm((W, E), F32),
                vm((2, C, J, E, E), BF16), vm((M, C, E), BF16), vm((M, C, E), BF16),
                vm((C, 2 * M, E), BF16),
                vm((H, 2 * M), BF16), vm((n_space, H, 2 * M), BF16), vm((2, H, 2 * M), F32),
                vm((16, 2 * M), F32), vm((n_tm, 16, 2 * M), F32), vm((8, 2 * M), F32),
                dma((6,)), dma((DC,)), dma((C,)), dma((2, 2, 2)), dma((2, 3)), dma((n_space,)), dma((n_space,)),
                dma((n_tm,)), dma((n_tm,)),
            ],
            compiler_params=pltpu.CompilerParams(
                collective_id=0, has_side_effects=True, vmem_limit_bytes=VMEM - room),
        )(density, active.reshape(2, H), neighbours.T, near_blocks, to_moments, from_moments,
          decay_rates.reshape(1, M), lengths.reshape(2, H))
        return pl.pallas_call(
            finish,
            out_shape=jax.ShapeDtypeStruct((T, C, E), BF16),
            in_specs=[vspec] * 4,
            out_specs=anyspec,
            scratch_shapes=[vm((T * 8, E), F32), vm((C // 8, T, 8, E), BF16), dma((C // 8,))],
            compiler_params=pltpu.CompilerParams(vmem_limit_bytes=16 * 1024 * 1024),
        )(*held)

    placed = (
        P("tm", "space", None), P("tm"), P("space", None), P(None, "space", None, None, None),
        P(None, "space", None), P(None, "space", None), P(), P("tm"),
    )
    return jax.shard_map(
        local, mesh=mesh, in_specs=placed, out_specs=P("tm", "space", None), check_vma=False)
```

```python
import functools
import math

import jax
import jax.numpy as jnp
from jax import lax
from jax.experimental import pallas as pl
from jax.experimental.pallas import tpu as pltpu
from jax.sharding import PartitionSpec as P

REACH = 8
U = 8
DC = 2
PAD = 16


def PIECES(T):
    return ((0, 4, 0, T // 2), (0, 4, T // 2, T // 2), (4, 2, 0, T), (6, 2, 0, T))


VMEM = 67043328
MESH = pl.DeviceIdType.MESH
F32, BF16 = jnp.float32, jnp.bfloat16


def spread(row):
    return jnp.broadcast_to(row, (128, row.shape[1])).T


def swap16():
    r = lax.broadcasted_iota(jnp.int32, (256, 256), 0)
    s = lax.broadcasted_iota(jnp.int32, (256, 256), 1)
    return jnp.where(s == (r % 16) * 16 + r // 16, 1.0, 0.0).astype(BF16)


def swap8():
    r = lax.broadcasted_iota(jnp.int32, (256, 256), 0)
    s = lax.broadcasted_iota(jnp.int32, (256, 256), 1)
    return jnp.where(s == (r % 8) * 32 + r // 8, 1.0, 0.0).astype(BF16)


def settle(near, from_v, cluster, scaled, act, perm, pot, out, head=None):
    T, E = near(0).shape
    for i in range(0, 8, 2):
        far = jnp.dot(scaled, jnp.concatenate([from_v(i), from_v(i + 1)], axis=1), preferred_element_type=F32)
        for u in range(2):
            live = (cluster + i + u).astype(F32) < act[...]
            x = near(i + u) + far[:, u * E:(u + 1) * E]
            if head is not None:
                head[i + u:i + u + 1, :] = x[0:1, :]
            pot[i + u] = jnp.where(live, x, 0.0).astype(BF16)
    for t in range(0, T, 64):
        x = [pot[:, t + i * 32:t + i * 32 + 32, :].reshape(256, E) for i in range(2)]
        y = jnp.dot(perm[...], jnp.concatenate(x, axis=1), preferred_element_type=F32)
        for i in range(2):
            out[t + i * 32:t + i * 32 + 32] = y[:, i * E:(i + 1) * E].reshape(32, 8, E).astype(BF16)


def kernel(n_tm, n_space, dens, active_h, nbrs_h, blocks, to_m, from_m, rates_h, lengths_h,
           near_far, from_far, act, scaled_o, ready_out, perm_out,
           near, from_v, pot, head, dens_v, work, active, nbrs, rates, lengths, perm,
           halo, row_out, row_pass, row_in, late_out, late_in, wb, to_raw, from_raw, to_v,
           part_out, part_swap, chip_out, part_in, keep, tot_out, tot_swap, tot_chip, tot_in,
           in_sem, dens_sem, w_sem, halo_sem, far_sem, swap_sem, row_sem, late_sem, part_ssem, part_rsem,
           tot_ssem, tot_rsem, ready):
    T, C, E = dens_v.shape
    M = to_raw.shape[0]
    J = wb.shape[2]
    H = T // 2
    tm, sp = lax.axis_index("tm"), lax.axis_index("space")
    first = sp * C
    one, nil = jnp.int32(1), jnp.int32(0)
    odd = lax.rem(sp, 2) == 1
    near_side = jnp.where(odd, nil, one)
    far_side = one - near_side
    chip = sp // 2
    n_chip = n_space // 2
    mate = sp + 2 * near_side - 1
    reach_lo = jnp.where(odd, nil, sp + 2)
    reach_hi = jnp.where(odd, sp - 1, jnp.int32(n_space))

    TD = T // DC
    small = [pltpu.make_async_copy(a, b, in_sem.at[2 + i]) for i, (a, b) in enumerate(
        ((active_h, active), (nbrs_h, nbrs), (rates_h, rates), (lengths_h, lengths)))]
    c_to = pltpu.make_async_copy(to_m, to_raw, in_sem.at[0])
    c_from = pltpu.make_async_copy(from_m, from_raw, in_sem.at[1])

    def c_dens(k):
        return pltpu.make_async_copy(dens.at[pl.ds(k * TD, TD)], dens_v.at[pl.ds(k * TD, TD)], dens_sem.at[k])

    small[0].start()
    for k in range(DC):
        c_dens(k).start()
    c_to.start()
    for c in small[1:]:
        c.start()
    c_from.start()
    barrier = pltpu.get_barrier_semaphore()

    def greet(t, s):
        pl.semaphore_signal(barrier, inc=1, device_id={"tm": t, "space": s}, device_id_type=MESH)

    for d in range(1, n_space):
        greet(tm, lax.rem(sp + d, n_space))

    @pl.loop(tm + 1, n_tm)
    def _(t):
        greet(t, sp)

        @pl.loop(reach_lo, reach_hi)
        def _(s):
            greet(t, s)

    def enter():
        pl.semaphore_wait(barrier, n_space - 1 + tm * n_chip)

        @pl.loop(0, tm)
        def _(t):
            for q in range(n_chip):
                s = jnp.where(chip == q, sp, jnp.where(chip > q, jnp.int32(2 * q), jnp.int32(2 * q + 1)))
                pl.semaphore_signal(ready, inc=1, device_id={"tm": t, "space": s}, device_id_type=MESH)

    def w_copy(c):
        return pltpu.make_async_copy(blocks.at[:, c], wb.at[:, c], w_sem.at[c])

    for lo, n in ((REACH, C - 2 * REACH), (near_side * (C - REACH), REACH), (far_side * (C - REACH), REACH)):
        @pl.loop(0, n)
        def _(i, lo=lo):
            w_copy(lo + i).start()

    perm[...] = swap16()
    perm_out[...] = swap8()
    small[0].wait()
    for h in range(2):
        act[h * H:(h + 1) * H, :] = spread(active[h:h + 1, :].astype(F32))

    def pair(raw, t, c0):
        x = [raw[pl.ds(t, 16), c0 + i * 16:c0 + i * 16 + 16, :].reshape(256, E) for i in range(2)]
        return jnp.dot(perm[...], jnp.concatenate(x, axis=1), preferred_element_type=F32)

    def expand(raw, dst):
        for b in range(M // 16):
            for c0 in range(0, C, 32):
                y = pair(raw, b * 16, c0).astype(BF16)
                for i in range(32):
                    x = y[i % 16 * 16:i % 16 * 16 + 16, i // 16 * E:(i // 16 + 1) * E]
                    dst[c0 + i, b * 16:b * 16 + 16, :] = x
                    dst[c0 + i, M + b * 16:M + b * 16 + 16, :] = x

    def mask(k):
        for t in range(k * TD, (k + 1) * TD, 16):
            live = act[t:t + 16, :]
            for c0 in range(0, C, 32):
                y = pair(dens_v, t, c0)
                for i in range(32):
                    x = y[i % 16 * 16:i % 16 * 16 + 16, i // 16 * E:(i // 16 + 1) * E]
                    x = jnp.where((first + (c0 + i)).astype(F32) < live, x, 0.0)
                    work[REACH + c0 + i, t:t + 16, :] = x.astype(BF16)

    far_there = jnp.where(odd, sp < n_space - 1, sp > 0)

    def near_copy(h):
        return pltpu.make_async_remote_copy(
            src_ref=work.at[pl.ds(REACH + near_side * (C - REACH), REACH), pl.ds(h * H, H), :],
            dst_ref=halo.at[far_side, :, pl.ds(h * H, H), :],
            send_sem=halo_sem.at[0, h], recv_sem=halo_sem.at[1, h],
            device_id={"tm": tm, "space": mate}, device_id_type=MESH)

    def far_copy(p, from_odd=None):
        a, n, lo, size = PIECES(T)[p]
        sender = odd if from_odd is None else from_odd
        src = REACH + jnp.where(odd, jnp.int32(C - a - n), jnp.int32(a))
        dst = jnp.where(sender, jnp.int32(REACH - a - n), jnp.int32(a))
        side = jnp.where(sender, nil, one)
        return pltpu.make_async_remote_copy(
            src_ref=work.at[pl.ds(src, n), pl.ds(lo, size), :],
            dst_ref=halo.at[side, pl.ds(dst, n), pl.ds(lo, size), :],
            send_sem=far_sem.at[0, p], recv_sem=far_sem.at[1, p],
            device_id={"tm": tm, "space": sp + 2 * far_side - 1}, device_id_type=MESH)

    def far_send(ps):
        @pl.when(far_there)
        def _():
            for p in ps:
                far_copy(p).start()

    @pl.when(tm > 0)
    def _():
        enter()

    c_dens(0).wait()
    mask(0)
    for k in range(1, DC):
        c_dens(k).wait()
    @pl.when(tm == 0)
    def _():
        enter()

    far_send((0,))
    near_copy(0).start()

    gid = lax.broadcasted_iota(jnp.int32, (C, E), 0).astype(F32) + first.astype(F32)
    row_out[...] = jnp.where(gid < act[T - 1:T, :], dens_v[T - 1].astype(F32), 0.0)
    for k in range(1, DC):
        mask(k)
    c_to.wait()
    expand(to_raw, to_v)
    far_send((1, 2, 3))
    near_copy(1).start()

    lane = lax.broadcasted_iota(jnp.int32, (H, 2 * M), 1)
    low = lane < M
    GB = 8
    moment = jnp.zeros((H, 2 * M), F32)
    for half in range(2):
        total = jnp.zeros((T, 2 * M), F32)
        for k in range(half * C // GB // 2, (half + 1) * C // GB // 2):
            a = jnp.concatenate([work[REACH + k * GB + i, 0:T, :] for i in range(GB)], axis=1)
            b = jnp.concatenate([to_v[k * GB + i] for i in range(GB)], axis=1)
            total = total + lax.dot_general(a, b, (((1,), (1,)), ((), ())), preferred_element_type=F32)
        moment = moment + jnp.where(low, total[0:H], total[H:T])

    small[2].wait()
    small[3].wait()
    r = rates[...]
    rr = jnp.concatenate([r, r], axis=1)
    span = jnp.where(low, spread(lengths[0:1, :]), spread(lengths[1:2, :]))
    fall = jnp.exp(-rr * span)
    pos = lax.broadcasted_iota(jnp.int32, (H, 2 * M), 0)
    d = 1
    while d < H:
        start = pos < d
        moment = fall * jnp.where(start, 0.0, pltpu.roll(moment, d, 0)) + moment
        fall = fall * jnp.where(start, 1.0, pltpu.roll(fall, d, 0))
        d *= 2
    end_b = jnp.broadcast_to(moment[H - 1:H, :], (8, 2 * M))
    end_a = jnp.broadcast_to(fall[H - 1:H, :], (8, 2 * M))
    low8 = low[0:8]
    roll_b, roll_a = pltpu.roll(end_b, M, 1), pltpu.roll(end_a, M, 1)
    tot_out[0:1] = (end_a * roll_a)[0:1]
    tot_out[1:2] = jnp.where(low8, roll_a * end_b + roll_b, end_a * roll_b + end_b)[0:1]
    moment = jnp.where(pos < 1, 0.0, pltpu.roll(moment, 1, 0))
    fall = jnp.where(pos < 1, 1.0, pltpu.roll(fall, 1, 0))
    moment = moment + fall * jnp.where(low8, 0.0, roll_b)[0:1]
    keep[0] = moment
    keep[1] = fall * jnp.where(low8, 1.0, roll_a)[0:1]
    part_out[...] = moment.astype(BF16)

    row_at = pl.multiple_of(jnp.where(odd, jnp.int32(C - REACH), nil), REACH)
    swaps = [pltpu.make_async_remote_copy(
        src_ref=a, dst_ref=b, send_sem=swap_sem.at[0, i], recv_sem=swap_sem.at[1, i],
        device_id={"tm": tm, "space": mate}, device_id_type=MESH) for i, (a, b) in enumerate(
            ((part_out, part_swap), (tot_out, tot_swap), (row_out.at[pl.ds(row_at, REACH)], row_pass)))]
    for c in swaps:
        c.start()

    first_row = lax.broadcasted_iota(jnp.int32, (T, E), 0) == 0
    small[1].wait()

    def near_field(c0, n, pad, dst, start=0):
        for u in range(n):
            w_copy(c0 + u).wait()
        for u in range(n):
            c = c0 + u
            rows = [jnp.clip(nbrs[j, c] - first + REACH, 0, C + 2 * REACH - 1) for j in range(J)]
            t = T + PAD if pad else T
            picked = jnp.concatenate([work[i, 0:t, :] for i in rows], axis=1)
            w = jnp.concatenate([wb[0, c].reshape(J * E, E), wb[1, c].reshape(J * E, E)], axis=1)
            both = jnp.dot(picked, w, preferred_element_type=F32)
            late = pltpu.roll(both[0:T, E:], 1, 0)
            if pad:
                late = jnp.where(first_row, both[T:T + 1, E:], late)
            else:
                late_out[pl.ds(c, 1), :] = late[0:1, :]
                late = jnp.where(first_row, 0.0, late)
            dst[c - start] = both[0:T, 0:E] + late

    near_field(REACH, U, False, near)

    for c in swaps:
        c.wait_recv()
    both = keep[0] + part_swap[...].astype(F32)
    keep[0] = both
    chip_out[...] = both.astype(BF16)
    tot_chip[0:1] = tot_out[0:1]
    tot_chip[1:2] = tot_out[1:2] + tot_swap[1:2]

    def part_copy(s):
        return pltpu.make_async_remote_copy(
            src_ref=chip_out, dst_ref=part_in.at[chip], send_sem=part_ssem.at[s], recv_sem=part_rsem.at[chip],
            device_id={"tm": tm, "space": s}, device_id_type=MESH)

    @pl.loop(reach_lo, reach_hi)
    def _(s):
        part_copy(s).start()

    def tot_copy(t, s):
        return pltpu.make_async_remote_copy(
            src_ref=tot_chip, dst_ref=tot_in.at[tm, chip], send_sem=tot_ssem.at[t, s], recv_sem=tot_rsem.at[tm, chip],
            device_id={"tm": t, "space": s}, device_id_type=MESH)

    more = tm < n_tm - 1
    less = tm > 0
    own_row = pltpu.make_async_remote_copy(
        src_ref=row_out, dst_ref=row_in.at[pl.ds(REACH, C)], send_sem=row_sem.at[0, 0], recv_sem=row_sem.at[1, 0],
        device_id={"tm": tm + 1, "space": sp}, device_id_type=MESH)
    pass_at = pl.multiple_of(jnp.where(odd, jnp.int32(REACH + C), nil), REACH)
    passes = jnp.logical_and(more, reach_lo < reach_hi)
    pass_row = pltpu.make_async_remote_copy(
        src_ref=row_pass, dst_ref=row_in.at[pl.ds(pass_at, REACH)], send_sem=row_sem.at[0, 1],
        recv_sem=row_sem.at[1, 1], device_id={"tm": tm + 1, "space": sp + 4 * near_side - 2}, device_id_type=MESH)

    def send_later():
        @pl.when(more)
        def _():
            pl.semaphore_wait(ready, (n_tm - 1 - tm) * (1 + reach_hi - reach_lo))

        @pl.when(more)
        def _():
            own_row.start()

        @pl.when(passes)
        def _():
            pass_row.start()

        @pl.loop(tm + 1, n_tm)
        def _(t):
            tot_copy(t, sp).start()

            @pl.loop(reach_lo, reach_hi)
            def _(s):
                tot_copy(t, s).start()

    @pl.when(less)
    def _():
        send_later()

    @pl.loop(1, (C - 2 * REACH) // U)
    def _(i):
        near_field(REACH + i * U, U, False, near)

    for h in range(2):
        near_copy(h).wait_recv()
    for g in range(REACH):
        work[near_side * (REACH + C) + g, 0:T, :] = halo[near_side, g]
    near_field(near_side * (C - REACH), REACH, False, near)

    @pl.when(tm == 0)
    def _():
        send_later()

    c_from.wait()
    expand(from_raw, from_v)

    def far_group(ps, pad):
        a, n = PIECES(T)[ps[0]][:2]

        @pl.when(far_there)
        def _():
            for p in ps:
                far_copy(p, jnp.logical_not(odd)).wait_recv()
            at = jnp.where(odd, jnp.int32(a), jnp.int32(REACH - a - n))
            for g in range(n):
                work[far_side * (REACH + C) + at + g, 0:T, :] = halo[far_side, at + g]

        near_field(jnp.where(odd, jnp.int32(C - REACH + a), jnp.int32(REACH - a - n)), n, pad, near_far,
                   far_side * (C - REACH))

    far_group((0, 1), False)
    late_copy = pltpu.make_async_remote_copy(
        src_ref=late_out, dst_ref=late_in, send_sem=late_sem.at[0], recv_sem=late_sem.at[1],
        device_id={"tm": tm + 1, "space": sp}, device_id_type=MESH)

    @pl.when(more)
    def _():
        late_copy.start()

    @pl.when(tm == 0)
    def _():
        row_in[...] = jnp.zeros_like(row_in)

    @pl.when(less)
    def _():
        own_row.wait_recv()

    @pl.when(jnp.logical_and(less, far_there))
    def _():
        pass_row.wait_recv()

    top = lax.broadcasted_iota(jnp.int32, (PAD, E), 0) == 0

    for i in range(3 * REACH):
        g = far_side * (C - REACH) + i
        r = jnp.broadcast_to(row_in[pl.ds(g, 1), :], (PAD, E))
        work[g, T:T + PAD, :] = jnp.where(top, r, 0.0).astype(BF16)

    far_group((2,), True)
    state = jnp.zeros((1, 2 * M), F32)
    keep[2, 0:1] = state

    @pl.loop(0, tm)
    def _(k):
        for q in range(n_chip):
            pltpu.make_async_remote_copy(
                src_ref=tot_chip, dst_ref=tot_in.at[k, q], send_sem=tot_ssem.at[k, q], recv_sem=tot_rsem.at[k, q],
                device_id={"tm": k, "space": sp}, device_id_type=MESH).wait_recv()
        gain = tot_in[k, 0, 1:2]
        for q in range(1, n_chip):
            gain = gain + tot_in[k, q, 1:2]
        keep[2, 0:1] = tot_in[k, 0, 0:1] * keep[2, 0:1] + gain

    far = keep[0]
    for d in range(1, n_chip):
        k = lax.rem(chip + d, n_chip)
        pltpu.make_async_remote_copy(
            src_ref=chip_out, dst_ref=part_in.at[k], send_sem=part_ssem.at[0], recv_sem=part_rsem.at[k],
            device_id={"tm": tm, "space": mate}, device_id_type=MESH).wait_recv()
        far = far + part_in[k].astype(F32)
    r = rates[...]
    root = jnp.sqrt(2.0 * jnp.concatenate([r, r], axis=1))
    scaled = (keep[1] * keep[2, 0:1] + far) * root
    scaled_o[0:H] = jnp.where(low, scaled, 0.0).astype(BF16)
    scaled_o[H:T] = jnp.where(low, 0.0, scaled).astype(BF16)

    base = near_side * REACH
    scaled = scaled_o[...]
    for b in range(C // 8 - 1):
        settle(lambda i, b=b: near[base + b * 8 + i], lambda i, b=b: from_v[base + b * 8 + i],
               first + base + b * 8, scaled, act, perm_out, pot.at[b], ready_out.at[b], head.at[b])
    for i in range(REACH):
        from_far[i] = from_v[far_side * (C - REACH) + i]

    far_group((3,), True)

    @pl.when(less)
    def _():
        late_copy.wait_recv()

        sub = lax.broadcasted_iota(jnp.int32, (8, E), 0)
        for b in range(C // 8 - 1):
            at = pl.multiple_of(base + b * 8, 8)
            x = head[b] + late_in[pl.ds(at, 8), :]
            live = (sub + (first + at)).astype(F32) < act[0:1, :]
            ready_out[b, 0] = jnp.where(live, x, 0.0).astype(BF16)
        n = PIECES(T)[0][1]
        for u in range(n):
            i = jnp.where(odd, jnp.int32(u), jnp.int32(REACH - n + u))
            near_far[i, 0:1, :] = near_far[i, 0:1, :] + late_in[pl.ds(far_side * (C - REACH) + i, 1), :]

    for c in swaps:
        c.wait_send()

    @pl.loop(reach_lo, reach_hi)
    def _(s):
        part_copy(s).wait_send()

    @pl.loop(tm + 1, n_tm)
    def _(t):
        tot_copy(t, sp).wait_send()

        @pl.loop(reach_lo, reach_hi)
        def _(s):
            tot_copy(t, s).wait_send()

    @pl.when(more)
    def _():
        late_copy.wait_send()

    @pl.when(more)
    def _():
        own_row.wait_send()

    @pl.when(passes)
    def _():
        pass_row.wait_send()

    for h in range(2):
        near_copy(h).wait_send()

    @pl.when(far_there)
    def _():
        for p in range(4):
            far_copy(p).wait_send()


def finish(near, from_v, act, scaled_o, ready, perm, out, pot, out_v, out_sem):
    T = near.shape[1]
    B = ready.shape[0]
    sp = lax.axis_index("space")
    odd = lax.rem(sp, 2) == 1
    one, nil = jnp.int32(1), jnp.int32(0)

    def out_copy(src, block, k, lo, n):
        at = pl.multiple_of(block * 8, 8)
        return pltpu.make_async_copy(src.at[pl.ds(lo, n)], out.at[pl.ds(lo, n), pl.ds(at, 8), :], out_sem.at[k])

    first = jnp.where(odd, nil, one)
    copies = [out_copy(ready.at[b], first + b, b, 0, T) for b in range(B)]
    for c in copies:
        c.start()
    block = jnp.where(odd, jnp.int32(B), nil)
    settle(lambda i: near[i], lambda i: from_v[i], (sp * (B + 1) + block) * 8, scaled_o[...], act, perm, pot, out_v)
    copies.append(out_copy(out_v, block, B, 0, T))
    copies[-1].start()
    for c in copies:
        c.wait()


def solution(mesh):
    n_tm, n_space = mesh.shape["tm"], mesh.shape["space"]

    def local(density, active, neighbours, near_blocks, to_moments, from_moments, decay_rates, lengths):
        T, C, E = density.shape
        J = neighbours.shape[1]
        M = decay_rates.shape[0]
        H, W = T // 2, C + 2 * REACH
        vm = lambda shape, t: pltpu.VMEM(shape, t)
        dma = pltpu.SemaphoreType.DMA
        kept = [((REACH, T, E), F32), ((REACH, 2 * M, E), BF16), ((T, 128), F32), ((T, 2 * M), BF16),
                ((C // 8 - 1, T, 8, E), BF16), ((256, 256), BF16)]
        room = sum(math.prod(s) * jnp.dtype(t).itemsize for s, t in kept) + 32 * 1024
        anyspec = pl.BlockSpec(memory_space=pl.ANY)
        vspec = pl.BlockSpec(memory_space=pltpu.VMEM)
        held = pl.pallas_call(
            functools.partial(kernel, n_tm, n_space),
            out_shape=[pltpu.VMEM(s, t) for s, t in kept],
            in_specs=[anyspec] * 8,
            out_specs=[vspec] * 6,
            scratch_shapes=[
                vm((C, T, E), F32), vm((C, 2 * M, E), BF16), vm((C // 8 - 1, 8, T, E), BF16),
                vm((C // 8 - 1, 8, E), F32),
                vm((T, C, E), BF16), vm((W, T + PAD, E), BF16),
                vm((2, H), jnp.int32), pltpu.SMEM((J, C), jnp.int32), vm((1, M), F32), vm((2, H), F32),
                vm((256, 256), BF16),
                vm((2, REACH, T, E), BF16), vm((C, E), F32), vm((REACH, E), F32), vm((W, E), F32), vm((C, E), F32),
                vm((C, E), F32),
                vm((2, C, J, E, E), BF16), vm((M, C, E), BF16), vm((M, C, E), BF16),
                vm((C, 2 * M, E), BF16),
                vm((H, 2 * M), BF16), vm((H, 2 * M), BF16), vm((H, 2 * M), BF16), vm((n_space // 2, H, 2 * M), BF16),
                vm((3, H, 2 * M), F32), vm((2, 2 * M), F32), vm((2, 2 * M), F32), vm((2, 2 * M), F32),
                vm((n_tm, n_space // 2, 2, 2 * M), F32),
                dma((6,)), dma((DC,)), dma((C,)), dma((2, 2)), dma((2, 4)), dma((2, 3)), dma((2, 2)), dma((2,)),
                dma((n_space,)), dma((n_space // 2,)), dma((n_tm, n_space)), dma((n_tm, n_space // 2)), pltpu.SemaphoreType.REGULAR,
            ],
            compiler_params=pltpu.CompilerParams(
                collective_id=0, has_side_effects=True, vmem_limit_bytes=VMEM - room),
        )(density, active.reshape(2, H), neighbours.T, near_blocks, to_moments, from_moments,
          decay_rates.reshape(1, M), lengths.reshape(2, H))
        return pl.pallas_call(
            finish,
            out_shape=jax.ShapeDtypeStruct((T, C, E), BF16),
            in_specs=[vspec] * 6,
            out_specs=anyspec,
            scratch_shapes=[vm((8, T, E), BF16), vm((T, 8, E), BF16), dma((C // 8,))],
            compiler_params=pltpu.CompilerParams(vmem_limit_bytes=16 * 1024 * 1024),
        )(*held)

    placed = (
        P("tm", "space", None), P("tm"), P("space", None), P(None, "space", None, None, None),
        P(None, "space", None), P(None, "space", None), P(), P("tm"),
    )
    return jax.shard_map(
        local, mesh=mesh, in_specs=placed, out_specs=P("tm", "space", None), check_vma=False)
```

```python
import functools
import math

import jax
import jax.numpy as jnp
from jax import lax
from jax.experimental import pallas as pl
from jax.experimental.pallas import tpu as pltpu
from jax.sharding import PartitionSpec as P

REACH = 8
U = 8
DC = 2
PAD = 16


def PIECES(T):
    return ((0, 4, 0, T // 2), (0, 4, T // 2, T // 2), (4, 4, 0, T))


VMEM = 67043328
MESH = pl.DeviceIdType.MESH
F32, BF16 = jnp.float32, jnp.bfloat16


def spread(row):
    return jnp.broadcast_to(row, (128, row.shape[1])).T


def swap16():
    r = lax.broadcasted_iota(jnp.int32, (256, 256), 0)
    s = lax.broadcasted_iota(jnp.int32, (256, 256), 1)
    return jnp.where(s == (r % 16) * 16 + r // 16, 1.0, 0.0).astype(BF16)


def swap8():
    r = lax.broadcasted_iota(jnp.int32, (256, 256), 0)
    s = lax.broadcasted_iota(jnp.int32, (256, 256), 1)
    return jnp.where(s == (r % 8) * 32 + r // 8, 1.0, 0.0).astype(BF16)


def settle(near, from_v, cluster, scaled, act, perm, pot, out, head=None):
    T, E = near(0).shape
    for i in range(0, 8, 2):
        far = jnp.dot(scaled, jnp.concatenate([from_v(i), from_v(i + 1)], axis=1), preferred_element_type=F32)
        for u in range(2):
            live = (cluster + i + u).astype(F32) < act[...]
            x = near(i + u) + far[:, u * E:(u + 1) * E]
            if head is not None:
                head[i + u:i + u + 1, :] = x[0:1, :]
            pot[i + u] = jnp.where(live, x, 0.0).astype(BF16)
    for t in range(0, T, 64):
        x = [pot[:, t + i * 32:t + i * 32 + 32, :].reshape(256, E) for i in range(2)]
        y = jnp.dot(perm[...], jnp.concatenate(x, axis=1), preferred_element_type=F32)
        for i in range(2):
            out[t + i * 32:t + i * 32 + 32] = y[:, i * E:(i + 1) * E].reshape(32, 8, E).astype(BF16)


def kernel(n_tm, n_space, dens, active_h, nbrs_h, blocks, to_m, from_m, rates_h, lengths_h,
           near_far, from_far, act, scaled_o, ready_out, perm_out,
           near, from_v, pot, head, dens_v, work, active, nbrs, rates, lengths, perm,
           halo, row_out, row_pass, row_in, late_out, late_in, wb, to_raw, from_raw, to_v,
           part_out, part_swap, chip_out, part_in, keep, tot_out, tot_swap, tot_chip, tot_in,
           in_sem, dens_sem, w_sem, halo_sem, far_sem, swap_sem, row_sem, late_sem, part_ssem, part_rsem,
           tot_ssem, tot_rsem, ready):
    T, C, E = dens_v.shape
    M = to_raw.shape[0]
    J = wb.shape[2]
    H = T // 2
    tm, sp = lax.axis_index("tm"), lax.axis_index("space")
    first = sp * C
    one, nil = jnp.int32(1), jnp.int32(0)
    odd = lax.rem(sp, 2) == 1
    near_side = jnp.where(odd, nil, one)
    far_side = one - near_side
    chip = sp // 2
    n_chip = n_space // 2
    mate = sp + 2 * near_side - 1
    reach_lo = jnp.where(odd, nil, sp + 2)
    reach_hi = jnp.where(odd, sp - 1, jnp.int32(n_space))

    TD = T // DC
    small = [pltpu.make_async_copy(a, b, in_sem.at[2 + i]) for i, (a, b) in enumerate(
        ((active_h, active), (nbrs_h, nbrs), (rates_h, rates), (lengths_h, lengths)))]
    c_to = pltpu.make_async_copy(to_m, to_raw, in_sem.at[0])
    c_from = pltpu.make_async_copy(from_m, from_raw, in_sem.at[1])

    def c_dens(k):
        return pltpu.make_async_copy(dens.at[pl.ds(k * TD, TD)], dens_v.at[pl.ds(k * TD, TD)], dens_sem.at[k])

    small[0].start()
    for k in range(DC):
        c_dens(k).start()
    c_to.start()
    for c in small[1:]:
        c.start()
    c_from.start()
    barrier = pltpu.get_barrier_semaphore()

    def greet(t, s):
        pl.semaphore_signal(barrier, inc=1, device_id={"tm": t, "space": s}, device_id_type=MESH)

    for d in range(1, n_space):
        greet(tm, lax.rem(sp + d, n_space))

    @pl.loop(tm + 1, n_tm)
    def _(t):
        greet(t, sp)

        @pl.loop(reach_lo, reach_hi)
        def _(s):
            greet(t, s)

    def enter():
        pl.semaphore_wait(barrier, n_space - 1 + tm * n_chip)

        @pl.loop(0, tm)
        def _(t):
            for q in range(n_chip):
                s = jnp.where(chip == q, sp, jnp.where(chip > q, jnp.int32(2 * q), jnp.int32(2 * q + 1)))
                pl.semaphore_signal(ready, inc=1, device_id={"tm": t, "space": s}, device_id_type=MESH)

    G = (C - 2 * REACH) // U
    HALF = REACH // 2
    near_lo = near_side * (C - REACH)
    far_lo = (far_side * (C - REACH) + jnp.where(odd, nil, jnp.int32(HALF)),
              far_side * (C - REACH) + jnp.where(odd, jnp.int32(HALF), nil))

    def w_copy(c, n, k):
        return pltpu.make_async_copy(blocks.at[:, pl.ds(c, n)], wb.at[:, pl.ds(c, n)], w_sem.at[k])

    @pl.loop(0, C - 2 * REACH)
    def _(i):
        w_copy(REACH + i, 1, i // U).start()

    for k, (lo, n) in enumerate(((near_lo, REACH), (far_lo[0], HALF), (far_lo[1], HALF))):
        @pl.loop(0, n)
        def _(i, lo=lo, k=k):
            w_copy(lo + i, 1, G + k).start()

    perm[...] = swap16()
    perm_out[...] = swap8()
    small[0].wait()
    for h in range(2):
        act[h * H:(h + 1) * H, :] = spread(active[h:h + 1, :].astype(F32))

    def pair(raw, t, c0):
        x = [raw[pl.ds(t, 16), c0 + i * 16:c0 + i * 16 + 16, :].reshape(256, E) for i in range(2)]
        return jnp.dot(perm[...], jnp.concatenate(x, axis=1), preferred_element_type=F32)

    def expand(raw, dst):
        for b in range(M // 16):
            for c0 in range(0, C, 32):
                y = pair(raw, b * 16, c0).astype(BF16)
                for i in range(32):
                    x = y[i % 16 * 16:i % 16 * 16 + 16, i // 16 * E:(i // 16 + 1) * E]
                    dst[c0 + i, b * 16:b * 16 + 16, :] = x
                    dst[c0 + i, M + b * 16:M + b * 16 + 16, :] = x

    def mask(k):
        for t in range(k * TD, (k + 1) * TD, 16):
            live = act[t:t + 16, :]
            for c0 in range(0, C, 32):
                y = pair(dens_v, t, c0)
                for i in range(32):
                    x = y[i % 16 * 16:i % 16 * 16 + 16, i // 16 * E:(i // 16 + 1) * E]
                    x = jnp.where((first + (c0 + i)).astype(F32) < live, x, 0.0)
                    work[REACH + c0 + i, t:t + 16, :] = x.astype(BF16)

    far_there = jnp.where(odd, sp < n_space - 1, sp > 0)

    def near_copy(lo, n):
        return pltpu.make_async_remote_copy(
            src_ref=work.at[pl.ds(REACH + near_side * (C - REACH), REACH), pl.ds(lo, n), :],
            dst_ref=halo.at[far_side, :, pl.ds(lo, n), :],
            send_sem=halo_sem.at[0], recv_sem=halo_sem.at[1],
            device_id={"tm": tm, "space": mate}, device_id_type=MESH)

    def far_copy(a, n, lo, size, k, from_odd=None):
        sender = odd if from_odd is None else from_odd
        src = REACH + jnp.where(odd, jnp.int32(C - a - n), jnp.int32(a))
        dst = jnp.where(sender, jnp.int32(REACH - a - n), jnp.int32(a))
        side = jnp.where(sender, nil, one)
        return pltpu.make_async_remote_copy(
            src_ref=work.at[pl.ds(src, n), pl.ds(lo, size), :],
            dst_ref=halo.at[side, pl.ds(dst, n), pl.ds(lo, size), :],
            send_sem=far_sem.at[0], recv_sem=far_sem.at[1 + k],
            device_id={"tm": tm, "space": sp + 2 * far_side - 1}, device_id_type=MESH)

    def far_send(ps):
        @pl.when(far_there)
        def _():
            for p in ps:
                far_copy(*PIECES(T)[p], PIECES(T)[p][0] // HALF).start()

    @pl.when(tm > 0)
    def _():
        enter()

    c_dens(0).wait()
    mask(0)
    for k in range(1, DC):
        c_dens(k).wait()
    @pl.when(tm == 0)
    def _():
        enter()

    far_send((0,))
    near_copy(0, H).start()

    gid = lax.broadcasted_iota(jnp.int32, (C, E), 0).astype(F32) + first.astype(F32)
    row_out[...] = jnp.where(gid < act[T - 1:T, :], dens_v[T - 1].astype(F32), 0.0)
    for k in range(1, DC):
        mask(k)
    c_to.wait()
    expand(to_raw, to_v)
    far_send((1, 2))
    near_copy(H, H).start()

    lane = lax.broadcasted_iota(jnp.int32, (H, 2 * M), 1)
    low = lane < M
    GB = 8
    moment = jnp.zeros((H, 2 * M), F32)
    for half in range(2):
        total = jnp.zeros((T, 2 * M), F32)
        for k in range(half * C // GB // 2, (half + 1) * C // GB // 2):
            a = jnp.concatenate([work[REACH + k * GB + i, 0:T, :] for i in range(GB)], axis=1)
            b = jnp.concatenate([to_v[k * GB + i] for i in range(GB)], axis=1)
            total = total + lax.dot_general(a, b, (((1,), (1,)), ((), ())), preferred_element_type=F32)
        moment = moment + jnp.where(low, total[0:H], total[H:T])

    small[2].wait()
    small[3].wait()
    r = rates[...]
    rr = jnp.concatenate([r, r], axis=1)
    span = jnp.where(low, spread(lengths[0:1, :]), spread(lengths[1:2, :]))
    fall = jnp.exp(-rr * span)
    pos = lax.broadcasted_iota(jnp.int32, (H, 2 * M), 0)
    d = 1
    while d < H:
        start = pos < d
        moment = fall * jnp.where(start, 0.0, pltpu.roll(moment, d, 0)) + moment
        fall = fall * jnp.where(start, 1.0, pltpu.roll(fall, d, 0))
        d *= 2
    end_b = jnp.broadcast_to(moment[H - 1:H, :], (8, 2 * M))
    end_a = jnp.broadcast_to(fall[H - 1:H, :], (8, 2 * M))
    low8 = low[0:8]
    roll_b, roll_a = pltpu.roll(end_b, M, 1), pltpu.roll(end_a, M, 1)
    tot_out[0:1] = (end_a * roll_a)[0:1]
    tot_out[1:2] = jnp.where(low8, roll_a * end_b + roll_b, end_a * roll_b + end_b)[0:1]
    moment = jnp.where(pos < 1, 0.0, pltpu.roll(moment, 1, 0))
    fall = jnp.where(pos < 1, 1.0, pltpu.roll(fall, 1, 0))
    moment = moment + fall * jnp.where(low8, 0.0, roll_b)[0:1]
    keep[0] = moment
    keep[1] = fall * jnp.where(low8, 1.0, roll_a)[0:1]
    part_out[...] = moment.astype(BF16)

    row_at = pl.multiple_of(jnp.where(odd, jnp.int32(C - REACH), nil), REACH)
    swaps = [pltpu.make_async_remote_copy(
        src_ref=a, dst_ref=b, send_sem=swap_sem.at[0, i], recv_sem=swap_sem.at[1, i],
        device_id={"tm": tm, "space": mate}, device_id_type=MESH) for i, (a, b) in enumerate(
            ((part_out, part_swap), (tot_out, tot_swap), (row_out.at[pl.ds(row_at, REACH)], row_pass)))]
    for c in swaps:
        c.start()

    first_row = lax.broadcasted_iota(jnp.int32, (T, E), 0) == 0
    small[1].wait()

    def near_field(c0, n, pad, dst, k, start=0):
        w_copy(c0, n, k).wait()
        for u in range(n):
            c = c0 + u
            rows = [jnp.clip(nbrs[j, c] - first + REACH, 0, C + 2 * REACH - 1) for j in range(J)]
            t = T + PAD if pad else T
            picked = jnp.concatenate([work[i, 0:t, :] for i in rows], axis=1)
            w = jnp.concatenate([wb[0, c].reshape(J * E, E), wb[1, c].reshape(J * E, E)], axis=1)
            both = jnp.dot(picked, w, preferred_element_type=F32)
            late = pltpu.roll(both[0:T, E:], 1, 0)
            if pad:
                late = jnp.where(first_row, both[T:T + 1, E:], late)
            else:
                late_out[pl.ds(c, 1), :] = late[0:1, :]
                late = jnp.where(first_row, 0.0, late)
            dst[c - start] = both[0:T, 0:E] + late

    near_field(REACH, U, False, near, 0)

    for c in swaps:
        c.wait_recv()
    both = keep[0] + part_swap[...].astype(F32)
    keep[0] = both
    chip_out[...] = both.astype(BF16)
    tot_chip[0:1] = tot_out[0:1]
    tot_chip[1:2] = tot_out[1:2] + tot_swap[1:2]

    def part_copy(s):
        return pltpu.make_async_remote_copy(
            src_ref=chip_out, dst_ref=part_in.at[chip], send_sem=part_ssem.at[s], recv_sem=part_rsem.at[chip],
            device_id={"tm": tm, "space": s}, device_id_type=MESH)

    @pl.loop(reach_lo, reach_hi)
    def _(s):
        part_copy(s).start()

    def tot_copy(t, s):
        return pltpu.make_async_remote_copy(
            src_ref=tot_chip, dst_ref=tot_in.at[tm, chip], send_sem=tot_ssem.at[t], recv_sem=tot_rsem.at[tm],
            device_id={"tm": t, "space": s}, device_id_type=MESH)

    more = tm < n_tm - 1
    less = tm > 0
    own_row = pltpu.make_async_remote_copy(
        src_ref=row_out, dst_ref=row_in.at[pl.ds(REACH, C)], send_sem=row_sem.at[0, 0], recv_sem=row_sem.at[1, 0],
        device_id={"tm": tm + 1, "space": sp}, device_id_type=MESH)
    pass_at = pl.multiple_of(jnp.where(odd, jnp.int32(REACH + C), nil), REACH)
    passes = jnp.logical_and(more, reach_lo < reach_hi)
    pass_row = pltpu.make_async_remote_copy(
        src_ref=row_pass, dst_ref=row_in.at[pl.ds(pass_at, REACH)], send_sem=row_sem.at[0, 1],
        recv_sem=row_sem.at[1, 1], device_id={"tm": tm + 1, "space": sp + 4 * near_side - 2}, device_id_type=MESH)

    def send_later():
        @pl.when(more)
        def _():
            pl.semaphore_wait(ready, (n_tm - 1 - tm) * (1 + reach_hi - reach_lo))

        @pl.when(more)
        def _():
            own_row.start()

        @pl.when(passes)
        def _():
            pass_row.start()

        @pl.loop(tm + 1, n_tm)
        def _(t):
            tot_copy(t, sp).start()

            @pl.loop(reach_lo, reach_hi)
            def _(s):
                tot_copy(t, s).start()

    @pl.when(less)
    def _():
        send_later()

    @pl.loop(1, (C - 2 * REACH) // U)
    def _(i):
        near_field(REACH + i * U, U, False, near, i)

    near_copy(0, T).wait_recv()
    for g in range(REACH):
        work[near_side * (REACH + C) + g, 0:T, :] = halo[near_side, g]
    near_field(near_lo, REACH, False, near, G)

    @pl.when(tm == 0)
    def _():
        send_later()

    c_from.wait()
    expand(from_raw, from_v)

    def far_group(k, pad):
        a = k * HALF

        @pl.when(far_there)
        def _():
            far_copy(a, HALF, 0, T, k, jnp.logical_not(odd)).wait_recv()
            at = jnp.where(odd, jnp.int32(a), jnp.int32(REACH - a - HALF))
            for g in range(HALF):
                work[far_side * (REACH + C) + at + g, 0:T, :] = halo[far_side, at + g]

        near_field(far_lo[k], HALF, pad, near_far, G + 1 + k, far_side * (C - REACH))

    far_group(0, False)
    late_copy = pltpu.make_async_remote_copy(
        src_ref=late_out, dst_ref=late_in, send_sem=late_sem.at[0], recv_sem=late_sem.at[1],
        device_id={"tm": tm + 1, "space": sp}, device_id_type=MESH)

    @pl.when(more)
    def _():
        late_copy.start()

    @pl.when(tm == 0)
    def _():
        row_in[...] = jnp.zeros_like(row_in)

    @pl.when(less)
    def _():
        own_row.wait_recv()

    @pl.when(jnp.logical_and(less, far_there))
    def _():
        pass_row.wait_recv()

    top = lax.broadcasted_iota(jnp.int32, (PAD, E), 0) == 0

    for i in range(3 * REACH):
        g = far_side * (C - REACH) + i
        r = jnp.broadcast_to(row_in[pl.ds(g, 1), :], (PAD, E))
        work[g, T:T + PAD, :] = jnp.where(top, r, 0.0).astype(BF16)

    state = jnp.zeros((1, 2 * M), F32)
    keep[2, 0:1] = state

    @pl.loop(0, tm)
    def _(k):
        pltpu.make_async_remote_copy(
            src_ref=tot_in.at[k], dst_ref=tot_in.at[k], send_sem=tot_ssem.at[k], recv_sem=tot_rsem.at[k],
            device_id={"tm": k, "space": sp}, device_id_type=MESH).wait_recv()
        gain = tot_in[k, 0, 1:2]
        for q in range(1, n_chip):
            gain = gain + tot_in[k, q, 1:2]
        keep[2, 0:1] = tot_in[k, 0, 0:1] * keep[2, 0:1] + gain

    far = keep[0]
    for d in range(1, n_chip):
        k = lax.rem(chip + d, n_chip)
        pltpu.make_async_remote_copy(
            src_ref=chip_out, dst_ref=part_in.at[k], send_sem=part_ssem.at[0], recv_sem=part_rsem.at[k],
            device_id={"tm": tm, "space": mate}, device_id_type=MESH).wait_recv()
        far = far + part_in[k].astype(F32)
    r = rates[...]
    root = jnp.sqrt(2.0 * jnp.concatenate([r, r], axis=1))
    scaled = (keep[1] * keep[2, 0:1] + far) * root
    scaled_o[0:H] = jnp.where(low, scaled, 0.0).astype(BF16)
    scaled_o[H:T] = jnp.where(low, 0.0, scaled).astype(BF16)

    base = near_side * REACH
    scaled = scaled_o[...]
    for b in range(C // 8 - 1):
        settle(lambda i, b=b: near[base + b * 8 + i], lambda i, b=b: from_v[base + b * 8 + i],
               first + base + b * 8, scaled, act, perm_out, pot.at[b], ready_out.at[b], head.at[b])
    for i in range(REACH):
        from_far[i] = from_v[far_side * (C - REACH) + i]

    far_group(1, True)

    @pl.when(less)
    def _():
        late_copy.wait_recv()

        sub = lax.broadcasted_iota(jnp.int32, (8, E), 0)
        for b in range(C // 8 - 1):
            at = pl.multiple_of(base + b * 8, 8)
            x = head[b] + late_in[pl.ds(at, 8), :]
            live = (sub + (first + at)).astype(F32) < act[0:1, :]
            ready_out[b, 0] = jnp.where(live, x, 0.0).astype(BF16)
        n = HALF
        for u in range(n):
            i = jnp.where(odd, jnp.int32(u), jnp.int32(REACH - n + u))
            near_far[i, 0:1, :] = near_far[i, 0:1, :] + late_in[pl.ds(far_side * (C - REACH) + i, 1), :]

    for c in swaps:
        c.wait_send()

    @pl.loop(reach_lo, reach_hi)
    def _(s):
        part_copy(s).wait_send()

    for j in range(n_chip):
        @pl.when(reach_hi - reach_lo == 2 * j)
        def _(j=j):
            @pl.loop(tm + 1, n_tm)
            def _(t):
                sent = tot_in.at[pl.ds(0, 1 + 2 * j), 0]
                pltpu.make_async_remote_copy(
                    src_ref=sent, dst_ref=sent, send_sem=tot_ssem.at[t], recv_sem=tot_rsem.at[t],
                    device_id={"tm": t, "space": sp}, device_id_type=MESH).wait_send()

    @pl.when(more)
    def _():
        late_copy.wait_send()

    @pl.when(more)
    def _():
        own_row.wait_send()

    @pl.when(passes)
    def _():
        pass_row.wait_send()

    near_copy(0, T).wait_send()

    @pl.when(far_there)
    def _():
        far_copy(0, REACH, 0, T, 0).wait_send()


def finish(near, from_v, act, scaled_o, ready, perm, out, pot, out_v, out_sem):
    T = near.shape[1]
    B = ready.shape[0]
    sp = lax.axis_index("space")
    odd = lax.rem(sp, 2) == 1
    one, nil = jnp.int32(1), jnp.int32(0)

    def out_copy(src, block, k, lo, n):
        at = pl.multiple_of(block * 8, 8)
        return pltpu.make_async_copy(src.at[pl.ds(lo, n)], out.at[pl.ds(lo, n), pl.ds(at, 8), :], out_sem.at[k])

    first = jnp.where(odd, nil, one)
    copies = [out_copy(ready.at[b], first + b, b, 0, T) for b in range(B)]
    for c in copies:
        c.start()
    block = jnp.where(odd, jnp.int32(B), nil)
    settle(lambda i: near[i], lambda i: from_v[i], (sp * (B + 1) + block) * 8, scaled_o[...], act, perm, pot, out_v)
    copies.append(out_copy(out_v, block, B, 0, T))
    copies[-1].start()
    for c in copies:
        c.wait()


def solution(mesh):
    n_tm, n_space = mesh.shape["tm"], mesh.shape["space"]

    def local(density, active, neighbours, near_blocks, to_moments, from_moments, decay_rates, lengths):
        T, C, E = density.shape
        J = neighbours.shape[1]
        M = decay_rates.shape[0]
        H, W = T // 2, C + 2 * REACH
        vm = lambda shape, t: pltpu.VMEM(shape, t)
        dma = pltpu.SemaphoreType.DMA
        kept = [((REACH, T, E), F32), ((REACH, 2 * M, E), BF16), ((T, 128), F32), ((T, 2 * M), BF16),
                ((C // 8 - 1, T, 8, E), BF16), ((256, 256), BF16)]
        room = sum(math.prod(s) * jnp.dtype(t).itemsize for s, t in kept) + 32 * 1024
        anyspec = pl.BlockSpec(memory_space=pl.ANY)
        vspec = pl.BlockSpec(memory_space=pltpu.VMEM)
        held = pl.pallas_call(
            functools.partial(kernel, n_tm, n_space),
            out_shape=[pltpu.VMEM(s, t) for s, t in kept],
            in_specs=[anyspec] * 8,
            out_specs=[vspec] * 6,
            scratch_shapes=[
                vm((C, T, E), F32), vm((C, 2 * M, E), BF16), vm((C // 8 - 1, 8, T, E), BF16),
                vm((C // 8 - 1, 8, E), F32),
                vm((T, C, E), BF16), vm((W, T + PAD, E), BF16),
                vm((2, H), jnp.int32), pltpu.SMEM((J, C), jnp.int32), vm((1, M), F32), vm((2, H), F32),
                vm((256, 256), BF16),
                vm((2, REACH, T, E), BF16), vm((C, E), F32), vm((REACH, E), F32), vm((W, E), F32), vm((C, E), F32),
                vm((C, E), F32),
                vm((2, C, J, E, E), BF16), vm((M, C, E), BF16), vm((M, C, E), BF16),
                vm((C, 2 * M, E), BF16),
                vm((H, 2 * M), BF16), vm((H, 2 * M), BF16), vm((H, 2 * M), BF16), vm((n_space // 2, H, 2 * M), BF16),
                vm((3, H, 2 * M), F32), vm((2, 2 * M), F32), vm((2, 2 * M), F32), vm((2, 2 * M), F32),
                vm((n_tm, n_space // 2, 2, 2 * M), F32),
                dma((6,)), dma((DC,)), dma(((C - 2 * REACH) // U + 3,)), dma((2,)), dma((3,)), dma((2, 3)), dma((2, 2)), dma((2,)),
                dma((n_space,)), dma((n_space // 2,)), dma((n_tm,)), dma((n_tm,)), pltpu.SemaphoreType.REGULAR,
            ],
            compiler_params=pltpu.CompilerParams(
                collective_id=0, has_side_effects=True, vmem_limit_bytes=VMEM - room),
        )(density, active.reshape(2, H), neighbours.T, near_blocks, to_moments, from_moments,
          decay_rates.reshape(1, M), lengths.reshape(2, H))
        return pl.pallas_call(
            finish,
            out_shape=jax.ShapeDtypeStruct((T, C, E), BF16),
            in_specs=[vspec] * 6,
            out_specs=anyspec,
            scratch_shapes=[vm((8, T, E), BF16), vm((T, 8, E), BF16), dma((C // 8,))],
            compiler_params=pltpu.CompilerParams(vmem_limit_bytes=16 * 1024 * 1024),
        )(*held)

    placed = (
        P("tm", "space", None), P("tm"), P("space", None), P(None, "space", None, None, None),
        P(None, "space", None), P(None, "space", None), P(), P("tm"),
    )
    return jax.shard_map(
        local, mesh=mesh, in_specs=placed, out_specs=P("tm", "space", None), check_vma=False)
```

```python
import functools
import math

import jax
import jax.numpy as jnp
from jax import lax
from jax.experimental import pallas as pl
from jax.experimental.pallas import tpu as pltpu
from jax.sharding import PartitionSpec as P

REACH = 8
U = 8
DC = 2
SPLIT = 4
PAD = 16


def PIECES(T):
    return ((0, 4, 0, T // 2), (0, 4, T // 2, T // 2), (4, 4, 0, T))


VMEM = 67043328
MESH = pl.DeviceIdType.MESH
F32, BF16 = jnp.float32, jnp.bfloat16


def spread(row):
    return jnp.broadcast_to(row, (128, row.shape[1])).T


def swap16():
    r = lax.broadcasted_iota(jnp.int32, (256, 256), 0)
    s = lax.broadcasted_iota(jnp.int32, (256, 256), 1)
    return jnp.where(s == (r % 16) * 16 + r // 16, 1.0, 0.0).astype(BF16)


def swap8():
    r = lax.broadcasted_iota(jnp.int32, (256, 256), 0)
    s = lax.broadcasted_iota(jnp.int32, (256, 256), 1)
    return jnp.where(s == (r % 8) * 32 + r // 8, 1.0, 0.0).astype(BF16)


def settle(near, from_v, cluster, scaled, act, perm, pot, out, head=None, sent=None):
    T, E = near(0).shape
    for i in range(0, 8, 2):
        far = jnp.dot(scaled, jnp.concatenate([from_v(i), from_v(i + 1)], axis=1), preferred_element_type=F32)
        for u in range(2):
            live = (cluster + i + u).astype(F32) < act[...]
            x = near(i + u) + far[:, u * E:(u + 1) * E]
            if head is not None:
                head[i + u:i + u + 1, :] = x[0:1, :]
            pot[i + u] = jnp.where(live, x, 0.0).astype(BF16)
    for t in range(0, T, 64):
        x = [pot[:, t + i * 32:t + i * 32 + 32, :].reshape(256, E) for i in range(2)]
        y = jnp.dot(perm[...], jnp.concatenate(x, axis=1), preferred_element_type=F32)
        for i in range(2):
            out[t + i * 32:t + i * 32 + 32] = y[:, i * E:(i + 1) * E].reshape(32, 8, E).astype(BF16)
        if sent is not None:
            sent(t, 64)


def kernel(n_tm, n_space, dens, active_h, nbrs_h, blocks, to_m, from_m, rates_h, lengths_h,
           near_far, from_far, act, scaled_o, ready_out, perm_out,
           near, from_v, pot, head, dens_v, work, active, nbrs, rates, lengths, perm,
           halo, row_out, row_pass, row_in, late_out, late_in, wb, to_raw, from_raw, to_v,
           part_out, part_swap, chip_out, part_in, keep, tot_out, tot_swap, tot_chip, tot_in,
           in_sem, dens_sem, w_sem, halo_sem, far_sem, swap_sem, row_sem, late_sem, part_sem,
           tot_ssem, tot_rsem, ready):
    T, C, E = dens_v.shape
    M = to_raw.shape[0]
    J = wb.shape[2]
    H = T // 2
    tm, sp = lax.axis_index("tm"), lax.axis_index("space")
    first = sp * C
    one, nil = jnp.int32(1), jnp.int32(0)
    odd = lax.rem(sp, 2) == 1
    near_side = jnp.where(odd, nil, one)
    far_side = one - near_side
    chip = sp // 2
    n_chip = n_space // 2
    mate = sp + 2 * near_side - 1
    reach_lo = jnp.where(odd, nil, sp + 2)
    reach_hi = jnp.where(odd, sp - 1, jnp.int32(n_space))

    TD = T // DC
    small = [pltpu.make_async_copy(a, b, in_sem.at[2 + i]) for i, (a, b) in enumerate(
        ((active_h, active), (nbrs_h, nbrs), (rates_h, rates), (lengths_h, lengths)))]
    c_to = pltpu.make_async_copy(to_m, to_raw, in_sem.at[0])
    c_from = pltpu.make_async_copy(from_m, from_raw, in_sem.at[1])

    def c_dens(k):
        return pltpu.make_async_copy(dens.at[pl.ds(k * TD, TD)], dens_v.at[pl.ds(k * TD, TD)], dens_sem.at[k])

    small[0].start()
    for k in range(DC):
        c_dens(k).start()
    c_to.start()
    for c in small[1:]:
        c.start()
    c_from.start()
    barrier = pltpu.get_barrier_semaphore()

    def greet(t, s):
        pl.semaphore_signal(barrier, inc=1, device_id={"tm": t, "space": s}, device_id_type=MESH)

    for d in range(1, n_space):
        greet(tm, lax.rem(sp + d, n_space))

    @pl.loop(tm + 1, n_tm)
    def _(t):
        greet(t, sp)

        @pl.loop(reach_lo, reach_hi)
        def _(s):
            greet(t, s)

    def enter():
        pl.semaphore_wait(barrier, n_space - 1 + tm * n_chip)

        @pl.loop(0, tm)
        def _(t):
            for q in range(n_chip):
                s = jnp.where(chip == q, sp, jnp.where(chip > q, jnp.int32(2 * q), jnp.int32(2 * q + 1)))
                pl.semaphore_signal(ready, inc=1, device_id={"tm": t, "space": s}, device_id_type=MESH)

    G = (C - 2 * REACH) // U
    HALF = REACH // 2
    near_lo = near_side * (C - REACH)
    far_lo = (far_side * (C - REACH) + jnp.where(odd, nil, jnp.int32(HALF)),
              far_side * (C - REACH) + jnp.where(odd, jnp.int32(HALF), nil))

    def w_copy(c, n, k):
        return pltpu.make_async_copy(blocks.at[:, pl.ds(c, n)], wb.at[:, pl.ds(c, n)], w_sem.at[k])

    @pl.loop(0, C - 2 * REACH)
    def _(i):
        w_copy(REACH + i, 1, i // U).start()

    for k, (lo, n) in enumerate(((near_lo, REACH), (far_lo[0], HALF), (far_lo[1], HALF))):
        @pl.loop(0, n)
        def _(i, lo=lo, k=k):
            w_copy(lo + i, 1, G + k).start()

    perm[...] = swap16()
    perm_out[...] = swap8()
    small[0].wait()
    for h in range(2):
        act[h * H:(h + 1) * H, :] = spread(active[h:h + 1, :].astype(F32))

    def pair(raw, t, c0):
        x = [raw[pl.ds(t, 16), c0 + i * 16:c0 + i * 16 + 16, :].reshape(256, E) for i in range(2)]
        return jnp.dot(perm[...], jnp.concatenate(x, axis=1), preferred_element_type=F32)

    def expand(raw, dst):
        for b in range(M // 16):
            for c0 in range(0, C, 32):
                y = pair(raw, b * 16, c0).astype(BF16)
                for i in range(32):
                    x = y[i % 16 * 16:i % 16 * 16 + 16, i // 16 * E:(i // 16 + 1) * E]
                    dst[c0 + i, b * 16:b * 16 + 16, :] = x
                    dst[c0 + i, M + b * 16:M + b * 16 + 16, :] = x

    def mask(k):
        for t in range(k * TD, (k + 1) * TD, 16):
            live = act[t:t + 16, :]
            for c0 in range(0, C, 32):
                y = pair(dens_v, t, c0)
                for i in range(32):
                    x = y[i % 16 * 16:i % 16 * 16 + 16, i // 16 * E:(i // 16 + 1) * E]
                    x = jnp.where((first + (c0 + i)).astype(F32) < live, x, 0.0)
                    work[REACH + c0 + i, t:t + 16, :] = x.astype(BF16)

    far_there = jnp.where(odd, sp < n_space - 1, sp > 0)

    def near_copy(lo, n):
        return pltpu.make_async_remote_copy(
            src_ref=work.at[pl.ds(REACH + near_side * (C - REACH), REACH), pl.ds(lo, n), :],
            dst_ref=halo.at[far_side, :, pl.ds(lo, n), :],
            send_sem=halo_sem.at[0], recv_sem=halo_sem.at[1],
            device_id={"tm": tm, "space": mate}, device_id_type=MESH)

    def far_copy(a, n, lo, size, k, from_odd=None):
        sender = odd if from_odd is None else from_odd
        src = REACH + jnp.where(odd, jnp.int32(C - a - n), jnp.int32(a))
        dst = jnp.where(sender, jnp.int32(REACH - a - n), jnp.int32(a))
        side = jnp.where(sender, nil, one)
        return pltpu.make_async_remote_copy(
            src_ref=work.at[pl.ds(src, n), pl.ds(lo, size), :],
            dst_ref=halo.at[side, pl.ds(dst, n), pl.ds(lo, size), :],
            send_sem=far_sem.at[0], recv_sem=far_sem.at[1 + k],
            device_id={"tm": tm, "space": sp + 2 * far_side - 1}, device_id_type=MESH)

    def far_send(ps):
        @pl.when(far_there)
        def _():
            for p in ps:
                far_copy(*PIECES(T)[p], PIECES(T)[p][0] // HALF).start()

    @pl.when(tm > 0)
    def _():
        enter()

    c_dens(0).wait()
    mask(0)
    for k in range(1, DC):
        c_dens(k).wait()
    @pl.when(tm == 0)
    def _():
        enter()

    far_send((0,))
    near_copy(0, H).start()

    gid = lax.broadcasted_iota(jnp.int32, (C, E), 0).astype(F32) + first.astype(F32)
    row_out[...] = jnp.where(gid < act[T - 1:T, :], dens_v[T - 1].astype(F32), 0.0)
    for k in range(1, DC):
        mask(k)
    c_to.wait()
    expand(to_raw, to_v)
    far_send((1, 2))
    near_copy(H, H).start()

    lane = lax.broadcasted_iota(jnp.int32, (H, 2 * M), 1)
    low = lane < M
    GB = 8
    moment = jnp.zeros((H, 2 * M), F32)
    for half in range(2):
        total = jnp.zeros((T, 2 * M), F32)
        for k in range(half * C // GB // 2, (half + 1) * C // GB // 2):
            a = jnp.concatenate([work[REACH + k * GB + i, 0:T, :] for i in range(GB)], axis=1)
            b = jnp.concatenate([to_v[k * GB + i] for i in range(GB)], axis=1)
            total = total + lax.dot_general(a, b, (((1,), (1,)), ((), ())), preferred_element_type=F32)
        moment = moment + jnp.where(low, total[0:H], total[H:T])

    small[2].wait()
    small[3].wait()
    r = rates[...]
    rr = jnp.concatenate([r, r], axis=1)
    span = jnp.where(low, spread(lengths[0:1, :]), spread(lengths[1:2, :]))
    fall = jnp.exp(-rr * span)
    pos = lax.broadcasted_iota(jnp.int32, (H, 2 * M), 0)
    d = 1
    while d < H:
        start = pos < d
        moment = fall * jnp.where(start, 0.0, pltpu.roll(moment, d, 0)) + moment
        fall = fall * jnp.where(start, 1.0, pltpu.roll(fall, d, 0))
        d *= 2
    end_b = jnp.broadcast_to(moment[H - 1:H, :], (8, 2 * M))
    end_a = jnp.broadcast_to(fall[H - 1:H, :], (8, 2 * M))
    low8 = low[0:8]
    roll_b, roll_a = pltpu.roll(end_b, M, 1), pltpu.roll(end_a, M, 1)
    tot_out[0:1] = (end_a * roll_a)[0:1]
    tot_out[1:2] = jnp.where(low8, roll_a * end_b + roll_b, end_a * roll_b + end_b)[0:1]
    moment = jnp.where(pos < 1, 0.0, pltpu.roll(moment, 1, 0))
    fall = jnp.where(pos < 1, 1.0, pltpu.roll(fall, 1, 0))
    moment = moment + fall * jnp.where(low8, 0.0, roll_b)[0:1]
    keep[0] = moment
    keep[1] = fall * jnp.where(low8, 1.0, roll_a)[0:1]
    part_out[...] = moment.astype(BF16)

    row_at = pl.multiple_of(jnp.where(odd, jnp.int32(C - REACH), nil), REACH)
    swaps = [pltpu.make_async_remote_copy(
        src_ref=a, dst_ref=b, send_sem=swap_sem.at[0, i], recv_sem=swap_sem.at[1, i],
        device_id={"tm": tm, "space": mate}, device_id_type=MESH) for i, (a, b) in enumerate(
            ((part_out, part_swap), (tot_out, tot_swap), (row_out.at[pl.ds(row_at, REACH)], row_pass)))]
    for c in swaps:
        c.start()

    first_row = lax.broadcasted_iota(jnp.int32, (T, E), 0) == 0
    small[1].wait()

    def near_field(c0, n, pad, dst, k, start=0):
        w_copy(c0, n, k).wait()
        for u in range(n):
            c = c0 + u
            rows = [jnp.clip(nbrs[j, c] - first + REACH, 0, C + 2 * REACH - 1) for j in range(J)]
            t = T + PAD if pad else T
            picked = jnp.concatenate([work[i, 0:t, :] for i in rows], axis=1)
            w = jnp.concatenate([wb[0, c].reshape(J * E, E), wb[1, c].reshape(J * E, E)], axis=1)
            both = jnp.dot(picked, w, preferred_element_type=F32)
            late = pltpu.roll(both[0:T, E:], 1, 0)
            if pad:
                late = jnp.where(first_row, both[T:T + 1, E:], late)
            else:
                late_out[pl.ds(c, 1), :] = late[0:1, :]
                late = jnp.where(first_row, 0.0, late)
            dst[c - start] = both[0:T, 0:E] + late

    near_field(REACH, U, False, near, 0)

    for c in swaps:
        c.wait_recv()
    both = keep[0] + part_swap[...].astype(F32)
    keep[0] = both
    chip_out[...] = both.astype(BF16)
    tot_chip[0:1] = tot_out[0:1]
    tot_chip[1:2] = tot_out[1:2] + tot_swap[1:2]

    def part_copy(s):
        return pltpu.make_async_remote_copy(
            src_ref=chip_out, dst_ref=part_in.at[chip], send_sem=part_sem.at[0], recv_sem=part_sem.at[1],
            device_id={"tm": tm, "space": s}, device_id_type=MESH)

    @pl.loop(reach_lo, reach_hi)
    def _(s):
        part_copy(s).start()

    def tot_copy(t, s):
        return pltpu.make_async_remote_copy(
            src_ref=tot_chip, dst_ref=tot_in.at[tm, chip], send_sem=tot_ssem.at[t], recv_sem=tot_rsem.at[0],
            device_id={"tm": t, "space": s}, device_id_type=MESH)

    more = tm < n_tm - 1
    less = tm > 0
    own_row = pltpu.make_async_remote_copy(
        src_ref=row_out, dst_ref=row_in.at[pl.ds(REACH, C)], send_sem=row_sem.at[0, 0], recv_sem=row_sem.at[1, 0],
        device_id={"tm": tm + 1, "space": sp}, device_id_type=MESH)
    pass_at = pl.multiple_of(jnp.where(odd, jnp.int32(REACH + C), nil), REACH)
    passes = jnp.logical_and(more, reach_lo < reach_hi)
    pass_row = pltpu.make_async_remote_copy(
        src_ref=row_pass, dst_ref=row_in.at[pl.ds(pass_at, REACH)], send_sem=row_sem.at[0, 1],
        recv_sem=row_sem.at[1, 1], device_id={"tm": tm + 1, "space": sp + 4 * near_side - 2}, device_id_type=MESH)

    def send_later():
        @pl.when(more)
        def _():
            pl.semaphore_wait(ready, (n_tm - 1 - tm) * (1 + reach_hi - reach_lo))

        @pl.when(more)
        def _():
            own_row.start()

        @pl.when(passes)
        def _():
            pass_row.start()

        @pl.loop(tm + 1, n_tm)
        def _(t):
            tot_copy(t, sp).start()

            @pl.loop(reach_lo, reach_hi)
            def _(s):
                tot_copy(t, s).start()

    @pl.when(less)
    def _():
        send_later()

    @pl.loop(1, (C - 2 * REACH) // U)
    def _(i):
        near_field(REACH + i * U, U, False, near, i)

    near_copy(0, T).wait_recv()
    for g in range(REACH):
        work[near_side * (REACH + C) + g, 0:T, :] = halo[near_side, g]
    near_field(near_lo, REACH, False, near, G)

    @pl.when(tm == 0)
    def _():
        send_later()

    c_from.wait()
    expand(from_raw, from_v)

    def far_group(k, pad):
        a = k * HALF

        @pl.when(far_there)
        def _():
            far_copy(a, HALF, 0, T, k, jnp.logical_not(odd)).wait_recv()
            at = jnp.where(odd, jnp.int32(a), jnp.int32(REACH - a - HALF))
            for g in range(HALF):
                work[far_side * (REACH + C) + at + g, 0:T, :] = halo[far_side, at + g]

        near_field(far_lo[k], HALF, pad, near_far, G + 1 + k, far_side * (C - REACH))

    far_group(0, False)
    late_copy = pltpu.make_async_remote_copy(
        src_ref=late_out, dst_ref=late_in, send_sem=late_sem.at[0], recv_sem=late_sem.at[1],
        device_id={"tm": tm + 1, "space": sp}, device_id_type=MESH)

    @pl.when(more)
    def _():
        late_copy.start()

    @pl.when(tm == 0)
    def _():
        row_in[...] = jnp.zeros_like(row_in)

    @pl.when(less)
    def _():
        own_row.wait_recv()

    @pl.when(jnp.logical_and(less, far_there))
    def _():
        pass_row.wait_recv()

    top = lax.broadcasted_iota(jnp.int32, (PAD, E), 0) == 0

    for i in range(3 * REACH):
        g = far_side * (C - REACH) + i
        r = jnp.broadcast_to(row_in[pl.ds(g, 1), :], (PAD, E))
        work[g, T:T + PAD, :] = jnp.where(top, r, 0.0).astype(BF16)

    state = jnp.zeros((1, 2 * M), F32)
    keep[2, 0:1] = state

    for j in range(1, n_tm):
        @pl.when(tm == j)
        def _(j=j):
            came = tot_in.at[pl.ds(0, j)]
            pltpu.make_async_remote_copy(
                src_ref=came, dst_ref=came, send_sem=tot_ssem.at[0], recv_sem=tot_rsem.at[0],
                device_id={"tm": tm - 1, "space": sp}, device_id_type=MESH).wait_recv()

    @pl.loop(0, tm)
    def _(k):
        gain = tot_in[k, 0, 1:2]
        for q in range(1, n_chip):
            gain = gain + tot_in[k, q, 1:2]
        keep[2, 0:1] = tot_in[k, 0, 0:1] * keep[2, 0:1] + gain

    far = keep[0]
    if n_chip > 1:
        came = part_in.at[pl.ds(0, n_chip - 1)]
        pltpu.make_async_remote_copy(
            src_ref=came, dst_ref=came, send_sem=part_sem.at[0], recv_sem=part_sem.at[1],
            device_id={"tm": tm, "space": mate}, device_id_type=MESH).wait_recv()
    for d in range(1, n_chip):
        far = far + part_in[lax.rem(chip + d, n_chip)].astype(F32)
    r = rates[...]
    root = jnp.sqrt(2.0 * jnp.concatenate([r, r], axis=1))
    scaled = (keep[1] * keep[2, 0:1] + far) * root
    scaled_o[0:H] = jnp.where(low, scaled, 0.0).astype(BF16)
    scaled_o[H:T] = jnp.where(low, 0.0, scaled).astype(BF16)

    base = near_side * REACH
    scaled = scaled_o[...]
    for b in range(C // 8 - 1):
        settle(lambda i, b=b: near[base + b * 8 + i], lambda i, b=b: from_v[base + b * 8 + i],
               first + base + b * 8, scaled, act, perm_out, pot.at[b], ready_out.at[b], head.at[b])
    for i in range(REACH):
        from_far[i] = from_v[far_side * (C - REACH) + i]

    far_group(1, True)

    @pl.when(less)
    def _():
        late_copy.wait_recv()

        sub = lax.broadcasted_iota(jnp.int32, (8, E), 0)
        for b in range(C // 8 - 1):
            at = pl.multiple_of(base + b * 8, 8)
            x = head[b] + late_in[pl.ds(at, 8), :]
            live = (sub + (first + at)).astype(F32) < act[0:1, :]
            ready_out[b, 0] = jnp.where(live, x, 0.0).astype(BF16)
        n = HALF
        for u in range(n):
            i = jnp.where(odd, jnp.int32(u), jnp.int32(REACH - n + u))
            near_far[i, 0:1, :] = near_far[i, 0:1, :] + late_in[pl.ds(far_side * (C - REACH) + i, 1), :]

    for c in swaps:
        c.wait_send()

    for j in range(n_chip):
        @pl.when(reach_hi - reach_lo == 2 * j)
        def _(j=j):
            if j > 0:
                sent = halo.at[0, pl.ds(0, j)]
                pltpu.make_async_remote_copy(
                    src_ref=sent, dst_ref=sent, send_sem=part_sem.at[0], recv_sem=part_sem.at[1],
                    device_id={"tm": tm, "space": mate}, device_id_type=MESH).wait_send()

            @pl.loop(tm + 1, n_tm)
            def _(t):
                sent = tot_in.at[pl.ds(0, 1 + 2 * j), 0]
                pltpu.make_async_remote_copy(
                    src_ref=sent, dst_ref=sent, send_sem=tot_ssem.at[t], recv_sem=tot_rsem.at[0],
                    device_id={"tm": t, "space": sp}, device_id_type=MESH).wait_send()

    @pl.when(more)
    def _():
        late_copy.wait_send()

    @pl.when(more)
    def _():
        own_row.wait_send()

    @pl.when(passes)
    def _():
        pass_row.wait_send()

    near_copy(0, T).wait_send()

    @pl.when(far_there)
    def _():
        far_copy(0, REACH, 0, T, 0).wait_send()


def finish(near, from_v, act, scaled_o, ready, perm, out, pot, out_v, out_sem):
    T = near.shape[1]
    B = ready.shape[0]
    sp = lax.axis_index("space")
    odd = lax.rem(sp, 2) == 1
    one, nil = jnp.int32(1), jnp.int32(0)

    def out_copy(src, block, k, lo, n):
        at = pl.multiple_of(block * 8, 8)
        return pltpu.make_async_copy(src.at[pl.ds(lo, n)], out.at[pl.ds(lo, n), pl.ds(at, 8), :], out_sem.at[k])

    first = jnp.where(odd, nil, one)
    for b in range(B):
        for lo in range(0, T, T // SPLIT):
            out_copy(ready.at[b], first + b, b, lo, T // SPLIT).start()
    block = jnp.where(odd, jnp.int32(B), nil)
    settle(lambda i: near[i], lambda i: from_v[i], (sp * (B + 1) + block) * 8, scaled_o[...], act, perm, pot, out_v,
           sent=lambda lo, n: out_copy(out_v, block, B, lo, n).start())
    for b in range(B):
        out_copy(ready.at[b], first + b, b, 0, T).wait()
    out_copy(out_v, block, B, 0, T).wait()


def solution(mesh):
    n_tm, n_space = mesh.shape["tm"], mesh.shape["space"]

    def local(density, active, neighbours, near_blocks, to_moments, from_moments, decay_rates, lengths):
        T, C, E = density.shape
        J = neighbours.shape[1]
        M = decay_rates.shape[0]
        H, W = T // 2, C + 2 * REACH
        vm = lambda shape, t: pltpu.VMEM(shape, t)
        dma = pltpu.SemaphoreType.DMA
        kept = [((REACH, T, E), F32), ((REACH, 2 * M, E), BF16), ((T, 128), F32), ((T, 2 * M), BF16),
                ((C // 8 - 1, T, 8, E), BF16), ((256, 256), BF16)]
        room = sum(math.prod(s) * jnp.dtype(t).itemsize for s, t in kept) + 32 * 1024
        anyspec = pl.BlockSpec(memory_space=pl.ANY)
        vspec = pl.BlockSpec(memory_space=pltpu.VMEM)
        held = pl.pallas_call(
            functools.partial(kernel, n_tm, n_space),
            out_shape=[pltpu.VMEM(s, t) for s, t in kept],
            in_specs=[anyspec] * 8,
            out_specs=[vspec] * 6,
            scratch_shapes=[
                vm((C, T, E), F32), vm((C, 2 * M, E), BF16), vm((C // 8 - 1, 8, T, E), BF16),
                vm((C // 8 - 1, 8, E), F32),
                vm((T, C, E), BF16), vm((W, T + PAD, E), BF16),
                vm((2, H), jnp.int32), pltpu.SMEM((J, C), jnp.int32), vm((1, M), F32), vm((2, H), F32),
                vm((256, 256), BF16),
                vm((2, REACH, T, E), BF16), vm((C, E), F32), vm((REACH, E), F32), vm((W, E), F32), vm((C, E), F32),
                vm((C, E), F32),
                vm((2, C, J, E, E), BF16), vm((M, C, E), BF16), vm((M, C, E), BF16),
                vm((C, 2 * M, E), BF16),
                vm((H, 2 * M), BF16), vm((H, 2 * M), BF16), vm((H, 2 * M), BF16), vm((n_space // 2, H, 2 * M), BF16),
                vm((3, H, 2 * M), F32), vm((2, 2 * M), F32), vm((2, 2 * M), F32), vm((2, 2 * M), F32),
                vm((n_tm, n_space // 2, 2, 2 * M), F32),
                dma((6,)), dma((DC,)), dma(((C - 2 * REACH) // U + 3,)), dma((2,)), dma((3,)), dma((2, 3)), dma((2, 2)), dma((2,)),
                dma((2,)), dma((n_tm,)), dma((1,)), pltpu.SemaphoreType.REGULAR,
            ],
            compiler_params=pltpu.CompilerParams(
                collective_id=0, has_side_effects=True, vmem_limit_bytes=VMEM - room),
        )(density, active.reshape(2, H), neighbours.T, near_blocks, to_moments, from_moments,
          decay_rates.reshape(1, M), lengths.reshape(2, H))
        return pl.pallas_call(
            finish,
            out_shape=jax.ShapeDtypeStruct((T, C, E), BF16),
            in_specs=[vspec] * 6,
            out_specs=anyspec,
            scratch_shapes=[vm((8, T, E), BF16), vm((T, 8, E), BF16), dma((C // 8,))],
            compiler_params=pltpu.CompilerParams(vmem_limit_bytes=16 * 1024 * 1024),
        )(*held)

    placed = (
        P("tm", "space", None), P("tm"), P("space", None), P(None, "space", None, None, None),
        P(None, "space", None), P(None, "space", None), P(), P("tm"),
    )
    return jax.shard_map(
        local, mesh=mesh, in_specs=placed, out_specs=P("tm", "space", None), check_vma=False)
```

```python
import functools
import math

import jax
import jax.numpy as jnp
from jax import lax
from jax.experimental import pallas as pl
from jax.experimental.pallas import tpu as pltpu
from jax.sharding import PartitionSpec as P

REACH = 8
U = 8
DC = 2
SPLIT = 4
PAD = 16


def PIECES(T):
    return ((0, 4, 0, T // 2), (0, 4, T // 2, T // 2), (4, 4, 0, T))


VMEM = 67043328
MESH = pl.DeviceIdType.MESH
F32, BF16 = jnp.float32, jnp.bfloat16


def spread(row):
    return jnp.broadcast_to(row, (128, row.shape[1])).T


def swap16():
    r = lax.broadcasted_iota(jnp.int32, (256, 256), 0)
    s = lax.broadcasted_iota(jnp.int32, (256, 256), 1)
    return jnp.where(s == (r % 16) * 16 + r // 16, 1.0, 0.0).astype(BF16)


def swap8():
    r = lax.broadcasted_iota(jnp.int32, (256, 256), 0)
    s = lax.broadcasted_iota(jnp.int32, (256, 256), 1)
    return jnp.where(s == (r % 8) * 32 + r // 8, 1.0, 0.0).astype(BF16)


def settle(near, from_v, cluster, scaled, act, perm, pot, out, head=None, sent=None):
    T, E = near(0).shape
    for i in range(0, 8, 2):
        far = jnp.dot(scaled, jnp.concatenate([from_v(i), from_v(i + 1)], axis=1), preferred_element_type=F32)
        for u in range(2):
            live = (cluster + i + u).astype(F32) < act[...]
            x = near(i + u) + far[:, u * E:(u + 1) * E]
            if head is not None:
                head[i + u:i + u + 1, :] = x[0:1, :]
            pot[i + u] = jnp.where(live, x, 0.0).astype(BF16)
    for t in range(0, T, 64):
        x = [pot[:, t + i * 32:t + i * 32 + 32, :].reshape(256, E) for i in range(2)]
        y = jnp.dot(perm[...], jnp.concatenate(x, axis=1), preferred_element_type=F32)
        for i in range(2):
            out[t + i * 32:t + i * 32 + 32] = y[:, i * E:(i + 1) * E].reshape(32, 8, E).astype(BF16)
        if sent is not None:
            sent(t, 64)


def kernel(n_tm, n_space, dens, active_h, nbrs_h, blocks, to_m, from_m, rates_h, lengths_h,
           near_far, from_far, act, scaled_o, ready_out, perm_out,
           near, from_v, pot, head, dens_v, work, active, nbrs, rates, lengths, perm,
           halo, row_out, row_pass, row_in, late_out, late_in, wb, to_raw, from_raw, to_v,
           part_out, part_swap, chip_out, part_in, keep, tot_out, tot_swap, tot_chip, tot_in,
           in_sem, dens_sem, w_sem, halo_sem, far_sem, swap_sem, row_sem, late_sem, part_sem,
           tot_ssem, tot_rsem, ready):
    T, C, E = dens_v.shape
    M = to_raw.shape[0]
    J = wb.shape[2]
    H = T // 2
    tm, sp = lax.axis_index("tm"), lax.axis_index("space")
    first = sp * C
    one, nil = jnp.int32(1), jnp.int32(0)
    odd = lax.rem(sp, 2) == 1
    near_side = jnp.where(odd, nil, one)
    far_side = one - near_side
    chip = sp // 2
    n_chip = n_space // 2
    mate = sp + 2 * near_side - 1
    reach_lo = jnp.where(odd, nil, sp + 2)
    reach_hi = jnp.where(odd, sp - 1, jnp.int32(n_space))

    TD = T // DC
    small = [pltpu.make_async_copy(a, b, in_sem.at[2 + i]) for i, (a, b) in enumerate(
        ((active_h, active), (nbrs_h, nbrs), (rates_h, rates), (lengths_h, lengths)))]
    c_to = pltpu.make_async_copy(to_m, to_raw, in_sem.at[0])
    c_from = pltpu.make_async_copy(from_m, from_raw, in_sem.at[1])

    def c_dens(k):
        return pltpu.make_async_copy(dens.at[pl.ds(k * TD, TD)], dens_v.at[pl.ds(k * TD, TD)], dens_sem.at[k])

    small[0].start()
    for k in range(DC):
        c_dens(k).start()
    c_to.start()
    for c in small[1:]:
        c.start()
    c_from.start()
    barrier = pltpu.get_barrier_semaphore()

    def greet(t, s):
        pl.semaphore_signal(barrier, inc=1, device_id={"tm": t, "space": s}, device_id_type=MESH)

    for d in range(1, n_space):
        greet(tm, lax.rem(sp + d, n_space))

    @pl.loop(tm + 1, n_tm)
    def _(t):
        greet(t, sp)

        @pl.loop(reach_lo, reach_hi)
        def _(s):
            greet(t, s)

    def enter():
        pl.semaphore_wait(barrier, n_space - 1 + tm * n_chip)

        @pl.loop(0, tm)
        def _(t):
            for q in range(n_chip):
                s = jnp.where(chip == q, sp, jnp.where(chip > q, jnp.int32(2 * q), jnp.int32(2 * q + 1)))
                pl.semaphore_signal(ready, inc=1, device_id={"tm": t, "space": s}, device_id_type=MESH)

    G = (C - 2 * REACH) // U
    HALF = REACH // 2
    near_lo = near_side * (C - REACH)
    far_lo = (far_side * (C - REACH) + jnp.where(odd, nil, jnp.int32(HALF)),
              far_side * (C - REACH) + jnp.where(odd, jnp.int32(HALF), nil))

    def w_copy(c, n, k):
        return pltpu.make_async_copy(blocks.at[:, pl.ds(c, n)], wb.at[:, pl.ds(c, n)], w_sem.at[k])

    @pl.loop(0, C - 2 * REACH)
    def _(i):
        w_copy(REACH + i, 1, i // U).start()

    for k, (lo, n) in enumerate(((near_lo, REACH), (far_lo[0], HALF), (far_lo[1], HALF))):
        @pl.loop(0, n)
        def _(i, lo=lo, k=k):
            w_copy(lo + i, 1, G + k).start()

    perm[...] = swap16()
    perm_out[...] = swap8()
    small[0].wait()
    for h in range(2):
        act[h * H:(h + 1) * H, :] = spread(active[h:h + 1, :].astype(F32))

    def pair(raw, t, c0):
        x = [raw[pl.ds(t, 16), c0 + i * 16:c0 + i * 16 + 16, :].reshape(256, E) for i in range(2)]
        return jnp.dot(perm[...], jnp.concatenate(x, axis=1), preferred_element_type=F32)

    def expand(raw, dst):
        for b in range(M // 16):
            for c0 in range(0, C, 32):
                y = pair(raw, b * 16, c0).astype(BF16)
                for i in range(32):
                    x = y[i % 16 * 16:i % 16 * 16 + 16, i // 16 * E:(i // 16 + 1) * E]
                    dst[c0 + i, b * 16:b * 16 + 16, :] = x
                    dst[c0 + i, M + b * 16:M + b * 16 + 16, :] = x

    def mask(k):
        for t in range(k * TD, (k + 1) * TD, 16):
            live = act[t:t + 16, :]
            for c0 in range(0, C, 32):
                y = pair(dens_v, t, c0)
                for i in range(32):
                    x = y[i % 16 * 16:i % 16 * 16 + 16, i // 16 * E:(i // 16 + 1) * E]
                    x = jnp.where((first + (c0 + i)).astype(F32) < live, x, 0.0)
                    work[REACH + c0 + i, t:t + 16, :] = x.astype(BF16)

    far_there = jnp.where(odd, sp < n_space - 1, sp > 0)

    def near_copy(lo, n):
        return pltpu.make_async_remote_copy(
            src_ref=work.at[pl.ds(REACH + near_side * (C - REACH), REACH), pl.ds(lo, n), :],
            dst_ref=halo.at[far_side, :, pl.ds(lo, n), :],
            send_sem=halo_sem.at[0], recv_sem=halo_sem.at[1],
            device_id={"tm": tm, "space": mate}, device_id_type=MESH)

    def far_copy(a, n, lo, size, k, from_odd=None):
        sender = odd if from_odd is None else from_odd
        src = REACH + jnp.where(odd, jnp.int32(C - a - n), jnp.int32(a))
        dst = jnp.where(sender, jnp.int32(REACH - a - n), jnp.int32(a))
        side = jnp.where(sender, nil, one)
        return pltpu.make_async_remote_copy(
            src_ref=work.at[pl.ds(src, n), pl.ds(lo, size), :],
            dst_ref=halo.at[side, pl.ds(dst, n), pl.ds(lo, size), :],
            send_sem=far_sem.at[0], recv_sem=far_sem.at[1 + k],
            device_id={"tm": tm, "space": sp + 2 * far_side - 1}, device_id_type=MESH)

    def far_send(ps):
        @pl.when(far_there)
        def _():
            for p in ps:
                far_copy(*PIECES(T)[p], PIECES(T)[p][0] // HALF).start()

    @pl.when(tm > 0)
    def _():
        enter()

    c_dens(0).wait()
    mask(0)
    for k in range(1, DC):
        c_dens(k).wait()
    @pl.when(tm == 0)
    def _():
        enter()

    near_copy(0, H).start()
    far_send((0,))

    gid = lax.broadcasted_iota(jnp.int32, (C, E), 0).astype(F32) + first.astype(F32)
    row_out[...] = jnp.where(gid < act[T - 1:T, :], dens_v[T - 1].astype(F32), 0.0)
    for k in range(1, DC):
        mask(k)
    c_to.wait()
    expand(to_raw, to_v)
    near_copy(H, H).start()
    far_send((1, 2))

    lane = lax.broadcasted_iota(jnp.int32, (H, 2 * M), 1)
    low = lane < M
    GB = 8
    moment = jnp.zeros((H, 2 * M), F32)
    for half in range(2):
        total = jnp.zeros((T, 2 * M), F32)
        for k in range(half * C // GB // 2, (half + 1) * C // GB // 2):
            a = jnp.concatenate([work[REACH + k * GB + i, 0:T, :] for i in range(GB)], axis=1)
            b = jnp.concatenate([to_v[k * GB + i] for i in range(GB)], axis=1)
            total = total + lax.dot_general(a, b, (((1,), (1,)), ((), ())), preferred_element_type=F32)
        moment = moment + jnp.where(low, total[0:H], total[H:T])

    small[2].wait()
    small[3].wait()
    r = rates[...]
    rr = jnp.concatenate([r, r], axis=1)
    span = jnp.where(low, spread(lengths[0:1, :]), spread(lengths[1:2, :]))
    fall = jnp.exp(-rr * span)
    pos = lax.broadcasted_iota(jnp.int32, (H, 2 * M), 0)
    d = 1
    while d < H:
        start = pos < d
        moment = fall * jnp.where(start, 0.0, pltpu.roll(moment, d, 0)) + moment
        fall = fall * jnp.where(start, 1.0, pltpu.roll(fall, d, 0))
        d *= 2
    end_b = jnp.broadcast_to(moment[H - 1:H, :], (8, 2 * M))
    end_a = jnp.broadcast_to(fall[H - 1:H, :], (8, 2 * M))
    low8 = low[0:8]
    roll_b, roll_a = pltpu.roll(end_b, M, 1), pltpu.roll(end_a, M, 1)
    tot_out[0:1] = (end_a * roll_a)[0:1]
    tot_out[1:2] = jnp.where(low8, roll_a * end_b + roll_b, end_a * roll_b + end_b)[0:1]
    moment = jnp.where(pos < 1, 0.0, pltpu.roll(moment, 1, 0))
    fall = jnp.where(pos < 1, 1.0, pltpu.roll(fall, 1, 0))
    moment = moment + fall * jnp.where(low8, 0.0, roll_b)[0:1]
    keep[0] = moment
    keep[1] = fall * jnp.where(low8, 1.0, roll_a)[0:1]
    part_out[...] = moment.astype(BF16)

    row_at = pl.multiple_of(jnp.where(odd, jnp.int32(C - REACH), nil), REACH)
    swaps = [pltpu.make_async_remote_copy(
        src_ref=a, dst_ref=b, send_sem=swap_sem.at[0, i], recv_sem=swap_sem.at[1, i],
        device_id={"tm": tm, "space": mate}, device_id_type=MESH) for i, (a, b) in enumerate(
            ((part_out, part_swap), (tot_out, tot_swap), (row_out.at[pl.ds(row_at, REACH)], row_pass)))]
    for c in swaps:
        c.start()

    first_row = lax.broadcasted_iota(jnp.int32, (T, E), 0) == 0
    small[1].wait()

    def near_field(c0, n, pad, dst, k, start=0):
        w_copy(c0, n, k).wait()
        for u in range(n):
            c = c0 + u
            rows = [jnp.clip(nbrs[j, c] - first + REACH, 0, C + 2 * REACH - 1) for j in range(J)]
            t = T + PAD if pad else T
            picked = jnp.concatenate([work[i, 0:t, :] for i in rows], axis=1)
            w = jnp.concatenate([wb[0, c].reshape(J * E, E), wb[1, c].reshape(J * E, E)], axis=1)
            both = jnp.dot(picked, w, preferred_element_type=F32)
            late = pltpu.roll(both[0:T, E:], 1, 0)
            if pad:
                late = jnp.where(first_row, both[T:T + 1, E:], late)
            else:
                late_out[pl.ds(c, 1), :] = late[0:1, :]
                late = jnp.where(first_row, 0.0, late)
            dst[c - start] = both[0:T, 0:E] + late

    near_field(REACH, U, False, near, 0)

    for c in swaps:
        c.wait_recv()
    both = keep[0] + part_swap[...].astype(F32)
    keep[0] = both
    chip_out[...] = both.astype(BF16)
    tot_chip[0:1] = tot_out[0:1]
    tot_chip[1:2] = tot_out[1:2] + tot_swap[1:2]

    def part_copy(s):
        return pltpu.make_async_remote_copy(
            src_ref=chip_out, dst_ref=part_in.at[chip], send_sem=part_sem.at[0], recv_sem=part_sem.at[1],
            device_id={"tm": tm, "space": s}, device_id_type=MESH)

    @pl.loop(reach_lo, reach_hi)
    def _(s):
        part_copy(s).start()

    def tot_copy(t, s):
        return pltpu.make_async_remote_copy(
            src_ref=tot_chip, dst_ref=tot_in.at[tm, chip], send_sem=tot_ssem.at[t], recv_sem=tot_rsem.at[0],
            device_id={"tm": t, "space": s}, device_id_type=MESH)

    more = tm < n_tm - 1
    less = tm > 0
    own_row = pltpu.make_async_remote_copy(
        src_ref=row_out, dst_ref=row_in.at[pl.ds(REACH, C)], send_sem=row_sem.at[0, 0], recv_sem=row_sem.at[1, 0],
        device_id={"tm": tm + 1, "space": sp}, device_id_type=MESH)
    pass_at = pl.multiple_of(jnp.where(odd, jnp.int32(REACH + C), nil), REACH)
    passes = jnp.logical_and(more, reach_lo < reach_hi)
    pass_row = pltpu.make_async_remote_copy(
        src_ref=row_pass, dst_ref=row_in.at[pl.ds(pass_at, REACH)], send_sem=row_sem.at[0, 1],
        recv_sem=row_sem.at[1, 1], device_id={"tm": tm + 1, "space": sp + 4 * near_side - 2}, device_id_type=MESH)

    def send_later():
        @pl.when(more)
        def _():
            pl.semaphore_wait(ready, (n_tm - 1 - tm) * (1 + reach_hi - reach_lo))

        @pl.when(more)
        def _():
            own_row.start()

        @pl.when(passes)
        def _():
            pass_row.start()

        @pl.loop(tm + 1, n_tm)
        def _(t):
            tot_copy(t, sp).start()

            @pl.loop(reach_lo, reach_hi)
            def _(s):
                tot_copy(t, s).start()

    @pl.when(less)
    def _():
        send_later()

    @pl.loop(1, (C - 2 * REACH) // U)
    def _(i):
        near_field(REACH + i * U, U, False, near, i)

    near_copy(0, T).wait_recv()
    for g in range(REACH):
        work[near_side * (REACH + C) + g, 0:T, :] = halo[near_side, g]
    near_field(near_lo, REACH, False, near, G)

    @pl.when(tm == 0)
    def _():
        send_later()

    c_from.wait()
    expand(from_raw, from_v)

    def far_group(k, pad):
        a = k * HALF

        @pl.when(far_there)
        def _():
            far_copy(a, HALF, 0, T, k, jnp.logical_not(odd)).wait_recv()
            at = jnp.where(odd, jnp.int32(a), jnp.int32(REACH - a - HALF))
            for g in range(HALF):
                work[far_side * (REACH + C) + at + g, 0:T, :] = halo[far_side, at + g]

        near_field(far_lo[k], HALF, pad, near_far, G + 1 + k, far_side * (C - REACH))

    far_group(0, False)
    late_copy = pltpu.make_async_remote_copy(
        src_ref=late_out, dst_ref=late_in, send_sem=late_sem.at[0], recv_sem=late_sem.at[1],
        device_id={"tm": tm + 1, "space": sp}, device_id_type=MESH)

    @pl.when(more)
    def _():
        late_copy.start()

    @pl.when(tm == 0)
    def _():
        row_in[...] = jnp.zeros_like(row_in)

    @pl.when(less)
    def _():
        own_row.wait_recv()

    @pl.when(jnp.logical_and(less, far_there))
    def _():
        pass_row.wait_recv()

    top = lax.broadcasted_iota(jnp.int32, (PAD, E), 0) == 0

    for i in range(3 * REACH):
        g = far_side * (C - REACH) + i
        r = jnp.broadcast_to(row_in[pl.ds(g, 1), :], (PAD, E))
        work[g, T:T + PAD, :] = jnp.where(top, r, 0.0).astype(BF16)

    state = jnp.zeros((1, 2 * M), F32)
    keep[2, 0:1] = state

    for j in range(1, n_tm):
        @pl.when(tm == j)
        def _(j=j):
            came = tot_in.at[pl.ds(0, j)]
            pltpu.make_async_remote_copy(
                src_ref=came, dst_ref=came, send_sem=tot_ssem.at[0], recv_sem=tot_rsem.at[0],
                device_id={"tm": tm - 1, "space": sp}, device_id_type=MESH).wait_recv()

    @pl.loop(0, tm)
    def _(k):
        gain = tot_in[k, 0, 1:2]
        for q in range(1, n_chip):
            gain = gain + tot_in[k, q, 1:2]
        keep[2, 0:1] = tot_in[k, 0, 0:1] * keep[2, 0:1] + gain

    far = keep[0]
    if n_chip > 1:
        came = part_in.at[pl.ds(0, n_chip - 1)]
        pltpu.make_async_remote_copy(
            src_ref=came, dst_ref=came, send_sem=part_sem.at[0], recv_sem=part_sem.at[1],
            device_id={"tm": tm, "space": mate}, device_id_type=MESH).wait_recv()
    for d in range(1, n_chip):
        far = far + part_in[lax.rem(chip + d, n_chip)].astype(F32)
    r = rates[...]
    root = jnp.sqrt(2.0 * jnp.concatenate([r, r], axis=1))
    scaled = (keep[1] * keep[2, 0:1] + far) * root
    scaled_o[0:H] = jnp.where(low, scaled, 0.0).astype(BF16)
    scaled_o[H:T] = jnp.where(low, 0.0, scaled).astype(BF16)

    base = near_side * REACH
    scaled = scaled_o[...]
    for b in range(C // 8 - 1):
        settle(lambda i, b=b: near[base + b * 8 + i], lambda i, b=b: from_v[base + b * 8 + i],
               first + base + b * 8, scaled, act, perm_out, pot.at[b], ready_out.at[b], head.at[b])
    for i in range(REACH):
        from_far[i] = from_v[far_side * (C - REACH) + i]

    far_group(1, True)

    @pl.when(less)
    def _():
        late_copy.wait_recv()

        sub = lax.broadcasted_iota(jnp.int32, (8, E), 0)
        for b in range(C // 8 - 1):
            at = pl.multiple_of(base + b * 8, 8)
            x = head[b] + late_in[pl.ds(at, 8), :]
            live = (sub + (first + at)).astype(F32) < act[0:1, :]
            ready_out[b, 0] = jnp.where(live, x, 0.0).astype(BF16)
        n = HALF
        for u in range(n):
            i = jnp.where(odd, jnp.int32(u), jnp.int32(REACH - n + u))
            near_far[i, 0:1, :] = near_far[i, 0:1, :] + late_in[pl.ds(far_side * (C - REACH) + i, 1), :]

    for c in swaps:
        c.wait_send()

    for j in range(n_chip):
        @pl.when(reach_hi - reach_lo == 2 * j)
        def _(j=j):
            if j > 0:
                sent = halo.at[0, pl.ds(0, j)]
                pltpu.make_async_remote_copy(
                    src_ref=sent, dst_ref=sent, send_sem=part_sem.at[0], recv_sem=part_sem.at[1],
                    device_id={"tm": tm, "space": mate}, device_id_type=MESH).wait_send()

            @pl.loop(tm + 1, n_tm)
            def _(t):
                sent = tot_in.at[pl.ds(0, 1 + 2 * j), 0]
                pltpu.make_async_remote_copy(
                    src_ref=sent, dst_ref=sent, send_sem=tot_ssem.at[t], recv_sem=tot_rsem.at[0],
                    device_id={"tm": t, "space": sp}, device_id_type=MESH).wait_send()

    @pl.when(more)
    def _():
        late_copy.wait_send()

    @pl.when(more)
    def _():
        own_row.wait_send()

    @pl.when(passes)
    def _():
        pass_row.wait_send()

    near_copy(0, T).wait_send()

    @pl.when(far_there)
    def _():
        far_copy(0, REACH, 0, T, 0).wait_send()


def finish(near, from_v, act, scaled_o, ready, perm, out, pot, out_v, out_sem):
    T = near.shape[1]
    B = ready.shape[0]
    sp = lax.axis_index("space")
    odd = lax.rem(sp, 2) == 1
    one, nil = jnp.int32(1), jnp.int32(0)

    def out_copy(src, block, k, lo, n):
        at = pl.multiple_of(block * 8, 8)
        return pltpu.make_async_copy(src.at[pl.ds(lo, n)], out.at[pl.ds(lo, n), pl.ds(at, 8), :], out_sem.at[k])

    first = jnp.where(odd, nil, one)
    for b in range(B):
        for lo in range(0, T, T // SPLIT):
            out_copy(ready.at[b], first + b, b, lo, T // SPLIT).start()
    block = jnp.where(odd, jnp.int32(B), nil)
    settle(lambda i: near[i], lambda i: from_v[i], (sp * (B + 1) + block) * 8, scaled_o[...], act, perm, pot, out_v,
           sent=lambda lo, n: out_copy(out_v, block, B, lo, n).start())
    for b in range(B):
        out_copy(ready.at[b], first + b, b, 0, T).wait()
    out_copy(out_v, block, B, 0, T).wait()


def solution(mesh):
    n_tm, n_space = mesh.shape["tm"], mesh.shape["space"]

    def local(density, active, neighbours, near_blocks, to_moments, from_moments, decay_rates, lengths):
        T, C, E = density.shape
        J = neighbours.shape[1]
        M = decay_rates.shape[0]
        H, W = T // 2, C + 2 * REACH
        vm = lambda shape, t: pltpu.VMEM(shape, t)
        dma = pltpu.SemaphoreType.DMA
        kept = [((REACH, T, E), F32), ((REACH, 2 * M, E), BF16), ((T, 128), F32), ((T, 2 * M), BF16),
                ((C // 8 - 1, T, 8, E), BF16), ((256, 256), BF16)]
        room = sum(math.prod(s) * jnp.dtype(t).itemsize for s, t in kept) + 32 * 1024
        anyspec = pl.BlockSpec(memory_space=pl.ANY)
        vspec = pl.BlockSpec(memory_space=pltpu.VMEM)
        held = pl.pallas_call(
            functools.partial(kernel, n_tm, n_space),
            out_shape=[pltpu.VMEM(s, t) for s, t in kept],
            in_specs=[anyspec] * 8,
            out_specs=[vspec] * 6,
            scratch_shapes=[
                vm((C, T, E), F32), vm((C, 2 * M, E), BF16), vm((C // 8 - 1, 8, T, E), BF16),
                vm((C // 8 - 1, 8, E), F32),
                vm((T, C, E), BF16), vm((W, T + PAD, E), BF16),
                vm((2, H), jnp.int32), pltpu.SMEM((J, C), jnp.int32), vm((1, M), F32), vm((2, H), F32),
                vm((256, 256), BF16),
                vm((2, REACH, T, E), BF16), vm((C, E), F32), vm((REACH, E), F32), vm((W, E), F32), vm((C, E), F32),
                vm((C, E), F32),
                vm((2, C, J, E, E), BF16), vm((M, C, E), BF16), vm((M, C, E), BF16),
                vm((C, 2 * M, E), BF16),
                vm((H, 2 * M), BF16), vm((H, 2 * M), BF16), vm((H, 2 * M), BF16), vm((n_space // 2, H, 2 * M), BF16),
                vm((3, H, 2 * M), F32), vm((2, 2 * M), F32), vm((2, 2 * M), F32), vm((2, 2 * M), F32),
                vm((n_tm, n_space // 2, 2, 2 * M), F32),
                dma((6,)), dma((DC,)), dma(((C - 2 * REACH) // U + 3,)), dma((2,)), dma((3,)), dma((2, 3)), dma((2, 2)), dma((2,)),
                dma((2,)), dma((n_tm,)), dma((1,)), pltpu.SemaphoreType.REGULAR,
            ],
            compiler_params=pltpu.CompilerParams(
                collective_id=0, has_side_effects=True, vmem_limit_bytes=VMEM - room),
        )(density, active.reshape(2, H), neighbours.T, near_blocks, to_moments, from_moments,
          decay_rates.reshape(1, M), lengths.reshape(2, H))
        return pl.pallas_call(
            finish,
            out_shape=jax.ShapeDtypeStruct((T, C, E), BF16),
            in_specs=[vspec] * 6,
            out_specs=anyspec,
            scratch_shapes=[vm((8, T, E), BF16), vm((T, 8, E), BF16), dma((C // 8,))],
            compiler_params=pltpu.CompilerParams(vmem_limit_bytes=16 * 1024 * 1024),
        )(*held)

    placed = (
        P("tm", "space", None), P("tm"), P("space", None), P(None, "space", None, None, None),
        P(None, "space", None), P(None, "space", None), P(), P("tm"),
    )
    return jax.shard_map(
        local, mesh=mesh, in_specs=placed, out_specs=P("tm", "space", None), check_vma=False)
```
